32 devices in a mesh: bins: 4 (over x, core), sta: 8 (over z, y).
Axes of the slice: x: 2, y: 2, z: 4, core: 2. Of those that a mesh axis runs over, the one named last changes fastest.
Arguments:
- spectra: bfloat16 [2, 128, 8, 2048], P(None, 'bins', None, 'sta'), may hold values from -110 to 110
- coords: int32 [2, 2048], replicated, may hold values from 0 to 2047
- slowness: int32 [2, 2048], replicated, may hold values from -32 to 31
Outputs:
- beam_power: float32 [128, 2048], P('bins', 'sta')
The draws below stay inside these ranges and needn't reach their ends.
All inputs are finite; a program needn't handle non-finite values.
Results may differ from the reference program's by a relative error of at most 0.002.
Values may be sent and summed in bfloat16 or wider, within the bound.
No kernel may reach another device: no remote copies, remote signals or barrier semaphores. Data moves between devices by JAX's collectives and lax.ppermute only.
A program may use at most 64 MiB of HBM per device.

```python
import math
import jax
import jax.numpy as jnp
from jax import lax

FREQS = 128
BEAMS = 2048
SEGS = 8
STATIONS = 2048


def draw_spectra(key, part):
    keys = jax.random.split(key, 3)
    levels = jnp.arange(FREQS, dtype=jnp.float32) / FREQS
    tilt = jnp.exp(jnp.log(4.0) * levels)
    seg_gain = jax.random.uniform(keys[1], (SEGS,), jnp.float32, 0.5, 1.5)
    noise = jnp.clip(jax.random.normal(keys[0], (2, FREQS, SEGS, STATIONS), jnp.float32), -3.0, 3.0)
    station_gain = jnp.exp(jax.random.uniform(keys[2], (STATIONS,), jnp.float32, jnp.log(0.5), jnp.log(2.0)))
    values = noise * tilt[None, :, None, None] * seg_gain[None, None, :, None] * station_gain[None, None, None, :]
    return values.astype(jnp.bfloat16)


def plant(entries, key, least, top_value):
    spot = [jax.random.randint(jax.random.fold_in(key, axis), (), 0, length) for axis, length in enumerate(entries.shape)]
    widest = entries.shape.index(max(entries.shape))
    next_to = spot[:widest] + [(spot[widest] + 1) % entries.shape[widest]] + spot[widest + 1:]
    return entries.at[tuple(spot)].set(least).at[tuple(next_to)].set(top_value)


def setup_inputs(seed: int = 0) -> dict:
    seeds = jax.random.split(jax.random.key(seed), 4)
    spectra = draw_spectra(jax.random.fold_in(seeds[3], 71), 0)
    coords = plant(jax.random.randint(seeds[1], (2, STATIONS), 0, 2048), jax.random.fold_in(seeds[1], 1), 0, 2047).astype(jnp.int32)
    slowness = plant(jax.random.randint(seeds[2], (2, BEAMS), -32, 32), jax.random.fold_in(seeds[2], 1), -32, 31).astype(jnp.int32)
    return {"spectra": spectra, "coords": coords, "slowness": slowness}


phase_modulus = 1048576
two_pi = 2.0 * math.pi
epsilon = 1e-06

def steering_table(delays, bin_number):
    phase_index = jnp.mod(bin_number * delays, phase_modulus)
    phase = phase_index.astype(jnp.float32) * (two_pi / phase_modulus)
    return jnp.concatenate([jnp.cos(phase), jnp.sin(phase)], 0).astype(jnp.bfloat16)

def reference(spectra, coords, slowness):
    values = spectra.astype(jnp.float32)
    sumsq = lax.optimization_barrier(jnp.sum(values * values, axis=(0, 1)))
    scale = jnp.sqrt(sumsq / (2 * FREQS) + epsilon)
    whitened = (values / scale).astype(jnp.bfloat16)
    delays = slowness[0][None, :] * coords[0][:, None] + slowness[1][None, :] * coords[1][:, None]

    def one_bin(pair_args):
        bin_white, bin_number = pair_args
        real_part = bin_white[0]
        imag_part = bin_white[1]
        upper_rows = jnp.concatenate([real_part, imag_part], 1)
        bottom = jnp.concatenate([imag_part, -imag_part * 0 - real_part], 1)
        stacked = jnp.concatenate([upper_rows, bottom], 0).astype(jnp.float32)
        steering = steering_table(delays, bin_number).astype(jnp.float32)
        amplitude = jnp.dot(stacked, steering, preferred_element_type=jnp.float32)
        return lax.optimization_barrier(jnp.sum(amplitude * amplitude, axis=0))
    bin_numbers = jnp.arange(1, FREQS + 1, dtype=jnp.int32)
    beam_power = lax.map(one_bin, (jnp.moveaxis(whitened, 1, 0), bin_numbers))
    return beam_power / (STATIONS * SEGS)
```

```python
import functools
import math

import jax
import jax.numpy as jnp
from jax import lax
from jax.experimental import pallas as pl
from jax.experimental.pallas import tpu as pltpu
from jax.sharding import PartitionSpec as P

phase_modulus = 1048576
two_pi = 2.0 * math.pi
epsilon = 1e-06
grid_low = -32
grid_size = 64
lane = 128


def cos_sin(index):
    quarter = phase_modulus // 4
    shift = quarter.bit_length() - 1
    turn = (index + quarter // 2) >> shift
    rest = index - (turn << shift)
    x = rest.astype(jnp.float32) * (two_pi / phase_modulus)
    y = x * x
    s = x + x * y * (-1 / 6 + y * (1 / 120 + y * (-1 / 5040 + y * (1 / 362880))))
    c = 1 + y * (-1 / 2 + y * (1 / 24 + y * (-1 / 720 + y * (1 / 40320))))
    odd = (turn & 1) == 1
    cos = jnp.where(odd, s, c)
    sin = jnp.where(odd, c, s)
    cos = jnp.where(((turn + 1) & 2) == 2, -cos, cos)
    sin = jnp.where((turn & 2) == 2, -sin, sin)
    return cos, sin


def kernel(first_ref, white_ref, coords_ref, slow_ref, out_ref, left, right, power):
    sources, bins, rows, width = white_ref.shape
    segs = rows // 2
    half = grid_size // 4
    norm = 1.0 / (sources * width * segs)
    sub = lax.broadcasted_iota(jnp.int32, (8, lane), 0)
    for f in range(bins):
        number = first_ref[0] + f
        for src in range(sources):
            for t in range(width // lane):
                at = pl.ds(src * width + t * lane, lane)
                east = jnp.broadcast_to(coords_ref[0:1, at], (8, lane)) * number
                north = jnp.broadcast_to(coords_ref[1:2, at], (8, lane)) * number
                ce, se = cos_sin(east)
                c8, _ = cos_sin(8 * north)
                step = 2 * c8
                tiles = [cos_sin(north * (sub + grid_low)), cos_sin(north * (sub + (grid_low + 8)))]
                for i in range(2, grid_size // 8):
                    tiles.append(tuple(step * a - b for a, b in zip(tiles[-1], tiles[-2])))
                for i in range(0, grid_size // 8, 2):
                    (c0, s0), (c1, s1) = tiles[i], tiles[i + 1]
                    here = pl.ds(8 * i, 16)
                    there = pl.ds(grid_size + 8 * i, 16)
                    right[f, here, at] = jnp.concatenate([c0, c1], 0).astype(jnp.bfloat16)
                    right[f, pl.ds(2 * grid_size + 8 * i, 16), at] = jnp.concatenate([s0, s1], 0).astype(jnp.bfloat16)
                    d0, d1 = c0 * ce - s0 * se, c1 * ce - s1 * se
                    r0, r1 = s0 * ce + c0 * se, s1 * ce + c1 * se
                    right[f, there, at] = jnp.concatenate([d0, d1], 0).astype(jnp.bfloat16)
                    right[f, pl.ds(3 * grid_size + 8 * i, 16), at] = jnp.concatenate([r0, r1], 0).astype(jnp.bfloat16)
                white = white_ref[src, f, :, pl.ds(t * lane, lane)]
                values = white.astype(jnp.float32)
                wr, wi = values[:segs], values[segs:]
                left[f, pl.ds(0, rows), at] = white
                ca, sa = 2 * ce * ce - 1, 2 * ce * se
                twice = 2 * ca
                cb, sb = jnp.ones_like(ca), jnp.zeros_like(sa)
                for a in range(1, half + 1):
                    base = rows * (2 * a - 1)
                    left[f, pl.ds(base, rows), at] = jnp.concatenate([wr * ca, wi * ca], 0).astype(jnp.bfloat16)
                    left[f, pl.ds(base + rows, rows), at] = jnp.concatenate([wr * sa, wi * sa], 0).astype(jnp.bfloat16)
                    ca, cb = twice * ca - cb, ca
                    sa, sb = twice * sa - sb, sa
        total = lax.dot_general(
            left[f], right[f], (((1,), (1,)), ((), ())), preferred_element_type=jnp.float32
        )

        def put(row, p, q):
            re = p[:, :lane] + q[:, lane:]
            im = q[:, :lane] - p[:, lane:]
            power[pl.ds(f * 2 * half + row, 1), :] = jnp.sum(re * re + im * im, axis=0, keepdims=True)

        put(half, total[:segs], total[segs:rows])
        for a in range(1, half + 1):
            base = rows * (2 * a - 1)
            cr, ci = total[base:base + segs], total[base + segs:base + rows]
            sr, si = total[base + rows:base + rows + segs], total[base + rows + segs:base + 2 * rows]
            put(half - a, cr - si, ci + sr)
            if a < half:
                put(half + a, cr + si, ci - sr)
    values = power[...] * norm
    high = values.astype(jnp.bfloat16)
    low = (values - high.astype(jnp.float32)).astype(jnp.bfloat16)
    pair = jnp.concatenate([high, low], 1)
    dests, _, beams = out_ref.shape
    for d in range(dests):
        at = pl.ds(d * beams, beams)
        east = slow_ref[0:1, at] - grid_low
        north = slow_ref[1:2, at] - grid_low
        column = (east & 1) * grid_size + north
        pick = lax.broadcasted_iota(jnp.int32, (lane, beams), 0) == column
        pick = jnp.where(pick, 1.0, 0.0).astype(jnp.bfloat16)
        found = jnp.dot(pair, jnp.concatenate([pick, pick], 0), preferred_element_type=jnp.float32)
        row = lax.broadcasted_iota(jnp.int32, (2 * half, beams), 0) == (east >> 1)
        for f in range(bins):
            part = jnp.where(row, found[f * 2 * half:(f + 1) * 2 * half], 0.0)
            out_ref[d, pl.ds(f, 1), :] = jnp.sum(part, axis=0, keepdims=True)


def beam_grid(first, white, coords, slowness, dests):
    sources, bins, rows, width = white.shape
    stations = sources * width
    beams = slowness.shape[1] // dests
    blocks = grid_size // 2 + 1
    vmem = pl.BlockSpec(memory_space=pltpu.VMEM)
    return pl.pallas_call(
        kernel,
        out_shape=jax.ShapeDtypeStruct((dests, bins, beams), jnp.float32),
        in_specs=[pl.BlockSpec(memory_space=pltpu.SMEM), vmem, vmem, vmem],
        out_specs=vmem,
        scratch_shapes=[
            pltpu.VMEM((bins, blocks * rows, stations), jnp.bfloat16),
            pltpu.VMEM((bins, 4 * grid_size, stations), jnp.bfloat16),
            pltpu.VMEM((bins * grid_size // 2, lane), jnp.float32),
        ],
        compiler_params=pltpu.CompilerParams(vmem_limit_bytes=48 * 1024 * 1024),
        name="beam_grid",
    )(first, white, coords, slowness)


def local(spectra, coords, slowness):
    bins_dev = spectra.shape[1]
    seg_count = spectra.shape[2]
    width = spectra.shape[3]
    peers = lax.axis_size("sta")
    groups = math.gcd(bins_dev, peers)
    copies = peers // groups
    bins_own = bins_dev // groups
    values = spectra.astype(jnp.float32)
    local_sq = jnp.sum(values * values, axis=(0, 1))
    total_bins = bins_dev * lax.axis_size("bins")
    totals = jnp.sum(lax.all_gather(local_sq, "bins"), axis=0)
    scale = jnp.sqrt(totals / (2 * total_bins) + epsilon)
    whitened = (values / scale).astype(jnp.bfloat16)
    parts = jnp.transpose(whitened.reshape(2, groups, bins_own, seg_count, width), (1, 2, 0, 3, 4))
    parts = parts.reshape(groups, bins_own, 2 * seg_count, width)
    if copies > 1:
        parts = jnp.repeat(parts, copies, axis=0)
    white = lax.all_to_all(parts, "sta", 0, 0, tiled=True)
    group = lax.axis_index("sta") // copies
    first = lax.axis_index("bins") * bins_dev + group * bins_own + 1
    powers = beam_grid(first.reshape(1).astype(jnp.int32), white, coords, slowness, peers)
    powers = lax.all_to_all(powers, "sta", 0, 0, tiled=True)
    return powers[::copies].reshape(bins_dev, -1)


def solution(mesh):
    in_specs = (P(None, "bins", None, "sta"), P(), P())
    out_specs = P("bins", "sta")
    return jax.shard_map(local, mesh=mesh, in_specs=in_specs, out_specs=out_specs, check_vma=False)
```

```python
import functools
import math

import jax
import jax.numpy as jnp
from jax import lax
from jax.experimental import pallas as pl
from jax.experimental.pallas import tpu as pltpu
from jax.sharding import PartitionSpec as P

phase_modulus = 1048576
two_pi = 2.0 * math.pi
epsilon = 1e-06
grid_low = -32
grid_size = 64
lane = 128
vmem_limit = 32 * 1024 * 1024


def cos_sin(index):
    quarter = phase_modulus // 4
    shift = quarter.bit_length() - 1
    turn = (index + quarter // 2) >> shift
    rest = index - (turn << shift)
    x = rest.astype(jnp.float32) * (two_pi / phase_modulus)
    y = x * x
    s = x + x * y * (-1 / 6 + y * (1 / 120 + y * (-1 / 5040 + y * (1 / 362880))))
    c = 1 + y * (-1 / 2 + y * (1 / 24 + y * (-1 / 720 + y * (1 / 40320))))
    odd = (turn & 1) == 1
    cos = jnp.where(odd, s, c)
    sin = jnp.where(odd, c, s)
    cos = jnp.where(((turn + 1) & 2) == 2, -cos, cos)
    sin = jnp.where((turn & 2) == 2, -sin, sin)
    return cos, sin


def tables_kernel(first_ref, coords_ref, right_ref, factor_ref):
    stations = right_ref.shape[2]
    number = first_ref[0] + pl.program_id(0)
    sub = lax.broadcasted_iota(jnp.int32, (8, lane), 0)
    half = grid_size // 4

    def one(t):
        at = pl.ds(pl.multiple_of(t * lane, lane), lane)
        east = jnp.broadcast_to(coords_ref[0:1, at], (8, lane)) * number
        north = jnp.broadcast_to(coords_ref[1:2, at], (8, lane)) * number
        for i in range(0, half, 16):
            low, high = (cos_sin(east * (2 * (sub + j) + 1)) for j in (i, i + 8))
            factor_ref[0, pl.ds(i, 16), at] = jnp.concatenate([low[0], high[0]], 0).astype(jnp.bfloat16)
            factor_ref[0, pl.ds(half + i, 16), at] = jnp.concatenate([low[1], high[1]], 0).astype(jnp.bfloat16)
        ce, se = cos_sin(east)
        c8, _ = cos_sin(8 * north)
        step = 2 * c8
        tiles = [cos_sin(north * (sub + grid_low)), cos_sin(north * (sub + (grid_low + 8)))]
        for i in range(2, grid_size // 8):
            tiles.append(tuple(step * a - b for a, b in zip(tiles[-1], tiles[-2])))
        for i in range(0, grid_size // 8, 2):
            (c0, s0), (c1, s1) = tiles[i], tiles[i + 1]
            turned = [
                (c0 * ce + s0 * se, c1 * ce + s1 * se),
                (c0, c1),
                (s0 * ce - c0 * se, s1 * ce - c1 * se),
                (s0, s1),
            ]
            for block, halves in enumerate(turned):
                rows = pl.ds(block * grid_size + 8 * i, 16)
                right_ref[0, rows, at] = jnp.concatenate(halves, 0).astype(jnp.bfloat16)

    @pl.loop(0, stations // lane // 4)
    def _(t):
        for u in range(4):
            one(t * 4 + u)


def tables(first, coords, bins):
    stations = coords.shape[1]
    vmem = pl.BlockSpec(memory_space=pltpu.VMEM)
    return pl.pallas_call(
        tables_kernel,
        out_shape=(
            pltpu.HBM((bins, 4 * grid_size, stations), jnp.bfloat16),
            jax.ShapeDtypeStruct((bins, grid_size // 2, stations), jnp.bfloat16),
        ),
        grid=(bins,),
        in_specs=[pl.BlockSpec(memory_space=pltpu.SMEM), vmem],
        out_specs=(
            pl.BlockSpec((1, 4 * grid_size, stations), lambda f: (f, 0, 0)),
            pl.BlockSpec((1, grid_size // 2, stations), lambda f: (f, 0, 0)),
        ),
        compiler_params=pltpu.CompilerParams(vmem_limit_bytes=vmem_limit),
        cost_estimate=pl.CostEstimate(flops=bins * stations * 4096, bytes_accessed=bins * stations * 576, transcendentals=0),
        name="tables",
    )(first, coords)


def kernel(white_ref, right_hbm, factor_ref, slow_hbm, out_ref, left, right, wide, power, slow_ref, arrived, slow_in):
    sources, bins, rows, width = white_ref.shape
    segs = rows // 2
    half = grid_size // 4
    step = math.gcd(width, 2 * lane)
    norm = 1.0 / (sources * width * segs)
    copies = {}
    for f in range(0, bins, 2):
        for src in range(sources):
            at = (pl.ds(f, min(2, bins - f)), slice(None), pl.ds(src * width, width))
            copies[f, src] = pltpu.make_async_copy(right_hbm.at[at], right.at[at], arrived.at[f // 2, src])
            copies[f, src].start()
    slow_copy = pltpu.make_async_copy(slow_hbm, slow_ref, slow_in)
    slow_copy.start()
    def finish(f, total):
        def square(p, q):
            re = p[:, :2 * grid_size] + q[:, 2 * grid_size:]
            im = q[:, :2 * grid_size] - p[:, 2 * grid_size:]
            return re * re + im * im

        plus, minus = 0.0, 0.0
        for g in range(segs):
            rc, rs = (total[2 * half * g + half * i:][:half] for i in (0, 1))
            ic, im = (total[2 * half * (segs + g) + half * i:][:half] for i in (0, 1))
            plus += square(rc + im, ic - rs)
            minus += square(rc - im, ic + rs)
        power[pl.ds(f * 2 * half, half), :] = plus
        power[pl.ds(f * 2 * half + half, half), :] = minus

    def build(f, src):
        for t in range(width // step):
            at = pl.ds(src * width + t * step, step)
            wide[f, :, at] = white_ref[src, f, :, pl.ds(t * step, step)].astype(jnp.float32)
            cos, sin = factor_ref[f, :half, at], factor_ref[f, half:, at]
            for r in range(rows):
                value = jnp.broadcast_to(wide[f, r:r + 1, at], (half, step)).astype(jnp.bfloat16)
                left[f, pl.ds(2 * half * r, half), at] = cos * value
                left[f, pl.ds(2 * half * r + half, half), at] = sin * value

    for f in range(0, bins, 2):
        both = range(f, min(f + 2, bins))
        totals = [0.0] * len(both)
        for src in range(sources):
            for i in both:
                build(i, src)
            copies[f, src].wait()
            at = pl.ds(src * width, width)
            for i in both:
                totals[i - f] += lax.dot_general(
                    left[i, :, at], right[i, :, at], (((1,), (1,)), ((), ())), preferred_element_type=jnp.float32
                )
        for i in both:
            finish(i, totals[i - f])
    slow_copy.wait()
    values = power[...] * norm
    high = values.astype(jnp.bfloat16)
    low = (values - high.astype(jnp.float32)).astype(jnp.bfloat16)
    pair = jnp.concatenate([high, low], 1)
    dests, _, beams = out_ref.shape
    for d in range(dests):
        at = pl.ds(d * beams, beams)
        east = slow_ref[0:1, at]
        north = slow_ref[1:2, at] - grid_low
        column = (east & 1) * grid_size + north
        pick = lax.broadcasted_iota(jnp.int32, (2 * grid_size, beams), 0) == column
        pick = jnp.where(pick, 1.0, 0.0).astype(jnp.bfloat16)
        found = jnp.dot(pair, jnp.concatenate([pick, pick], 0), preferred_element_type=jnp.float32)
        east = jnp.where(east >= 0, east >> 1, half - 1 - (east >> 1))
        row = lax.broadcasted_iota(jnp.int32, (2 * half, beams), 0) == east
        for f in range(bins):
            part = jnp.where(row, found[f * 2 * half:(f + 1) * 2 * half], 0.0)
            out_ref[d, pl.ds(f, 1), :] = jnp.sum(part, axis=0, keepdims=True)


def beam_grid(white, right, factor, slowness, dests):
    sources, bins, rows, width = white.shape
    stations = sources * width
    beams = slowness.shape[1] // dests
    vmem = pl.BlockSpec(memory_space=pltpu.VMEM)
    hbm = pl.BlockSpec(memory_space=pltpu.HBM)
    pin = pltpu.with_memory_space_constraint
    return pl.pallas_call(
        kernel,
        out_shape=jax.ShapeDtypeStruct((dests, bins, beams), jnp.float32),
        in_specs=[vmem, hbm, vmem, hbm],
        out_specs=vmem,
        scratch_shapes=[
            pltpu.VMEM((bins, grid_size // 2 * rows, stations), jnp.bfloat16),
            pltpu.VMEM((bins, 4 * grid_size, stations), jnp.bfloat16),
            pltpu.VMEM((bins, rows, stations), jnp.float32),
            pltpu.VMEM((bins * grid_size // 2, 2 * grid_size), jnp.float32),
            pltpu.VMEM(slowness.shape, jnp.int32),
            pltpu.SemaphoreType.DMA((pl.cdiv(bins, 2), sources)),
            pltpu.SemaphoreType.DMA,
        ],
        compiler_params=pltpu.CompilerParams(vmem_limit_bytes=vmem_limit),
        cost_estimate=pl.CostEstimate(flops=bins * stations * 4096, bytes_accessed=bins * stations * 576, transcendentals=0),
        name="beam_grid",
    )(white, pin(right, pltpu.HBM), factor, pin(slowness, pltpu.HBM))


def local(spectra, coords, slowness):
    bins_dev = spectra.shape[1]
    seg_count = spectra.shape[2]
    width = spectra.shape[3]
    peers = lax.axis_size("sta")
    groups = math.gcd(bins_dev, peers)
    copies = peers // groups
    bins_own = bins_dev // groups
    values = spectra.astype(jnp.float32)
    local_sq = jnp.sum(values * values, axis=(0, 1))
    total_bins = bins_dev * lax.axis_size("bins")
    totals = jnp.sum(lax.all_gather(local_sq, "bins"), axis=0)
    scale = jnp.sqrt(totals / (2 * total_bins) + epsilon)
    whitened = (values / scale).astype(jnp.bfloat16)
    parts = jnp.transpose(whitened.reshape(2, groups, bins_own, seg_count, width), (1, 2, 0, 3, 4))
    parts = parts.reshape(groups, bins_own, 2 * seg_count, width)
    if copies > 1:
        parts = jnp.repeat(parts, copies, axis=0)
    white = lax.all_to_all(parts, "sta", 0, 0, tiled=True)
    group = lax.axis_index("sta") // copies
    first = lax.axis_index("bins") * bins_dev + group * bins_own + 1
    right, factor = tables(first.reshape(1).astype(jnp.int32), coords, bins_own)
    powers = beam_grid(white, right, factor, slowness, peers)
    powers = lax.all_to_all(powers, "sta", 0, 0, tiled=True)
    return powers[::copies].reshape(bins_dev, -1)


def solution(mesh):
    in_specs = (P(None, "bins", None, "sta"), P(), P())
    out_specs = P("bins", "sta")
    return jax.shard_map(local, mesh=mesh, in_specs=in_specs, out_specs=out_specs, check_vma=False)
```

```python
import functools
import math

import jax
import jax.numpy as jnp
from jax import lax
from jax.experimental import pallas as pl
from jax.experimental.pallas import tpu as pltpu
from jax.sharding import PartitionSpec as P

phase_modulus = 1048576
two_pi = 2.0 * math.pi
epsilon = 1e-06
grid_low = -32
grid_size = 64
lane = 128
vmem_limit = 32 * 1024 * 1024


def cos_sin(index):
    quarter = phase_modulus // 4
    shift = quarter.bit_length() - 1
    turn = (index + quarter // 2) >> shift
    rest = index - (turn << shift)
    x = rest.astype(jnp.float32) * (two_pi / phase_modulus)
    y = x * x
    s = x + x * y * (-1 / 6 + y * (1 / 120 + y * (-1 / 5040 + y * (1 / 362880))))
    c = 1 + y * (-1 / 2 + y * (1 / 24 + y * (-1 / 720 + y * (1 / 40320))))
    odd = (turn & 1) == 1
    cos = jnp.where(odd, s, c)
    sin = jnp.where(odd, c, s)
    cos = jnp.where(((turn + 1) & 2) == 2, -cos, cos)
    sin = jnp.where((turn & 2) == 2, -sin, sin)
    return cos, sin


def tables_kernel(first_ref, coords_ref, right_ref, factor_ref):
    stations = right_ref.shape[2]
    number = first_ref[0] + pl.program_id(0)
    sub = lax.broadcasted_iota(jnp.int32, (8, lane), 0)
    half = grid_size // 4

    def one(t):
        at = pl.ds(pl.multiple_of(t * lane, lane), lane)
        east = jnp.broadcast_to(coords_ref[0:1, at], (8, lane)) * number
        north = jnp.broadcast_to(coords_ref[1:2, at], (8, lane)) * number
        for i in range(0, half, 16):
            low, high = (cos_sin(east * (2 * (sub + j) + 1)) for j in (i, i + 8))
            factor_ref[0, pl.ds(i, 16), at] = jnp.concatenate([low[0], high[0]], 0).astype(jnp.bfloat16)
            factor_ref[0, pl.ds(half + i, 16), at] = jnp.concatenate([low[1], high[1]], 0).astype(jnp.bfloat16)
        ce, se = cos_sin(east)
        c8, _ = cos_sin(8 * north)
        step = 2 * c8
        tiles = [cos_sin(north * (sub + grid_low)), cos_sin(north * (sub + (grid_low + 8)))]
        for i in range(2, grid_size // 8):
            tiles.append(tuple(step * a - b for a, b in zip(tiles[-1], tiles[-2])))
        for i in range(0, grid_size // 8, 2):
            (c0, s0), (c1, s1) = tiles[i], tiles[i + 1]
            turned = [
                (c0 * ce + s0 * se, c1 * ce + s1 * se),
                (c0, c1),
                (s0 * ce - c0 * se, s1 * ce - c1 * se),
                (s0, s1),
            ]
            for block, halves in enumerate(turned):
                rows = pl.ds(block * grid_size + 8 * i, 16)
                right_ref[0, rows, at] = jnp.concatenate(halves, 0).astype(jnp.bfloat16)

    @pl.loop(0, stations // lane // 4)
    def _(t):
        for u in range(4):
            one(t * 4 + u)


def tables(first, coords, bins):
    stations = coords.shape[1]
    vmem = pl.BlockSpec(memory_space=pltpu.VMEM)
    return pl.pallas_call(
        tables_kernel,
        out_shape=(
            jax.ShapeDtypeStruct((bins, 4 * grid_size, stations), jnp.bfloat16),
            jax.ShapeDtypeStruct((bins, grid_size // 2, stations), jnp.bfloat16),
        ),
        grid=(bins,),
        in_specs=[pl.BlockSpec(memory_space=pltpu.SMEM), vmem],
        out_specs=(
            pl.BlockSpec((1, 4 * grid_size, stations), lambda f: (f, 0, 0)),
            pl.BlockSpec((1, grid_size // 2, stations), lambda f: (f, 0, 0)),
        ),
        compiler_params=pltpu.CompilerParams(vmem_limit_bytes=vmem_limit),
        cost_estimate=pl.CostEstimate(flops=bins * stations * 4096, bytes_accessed=bins * stations * 576, transcendentals=0),
        name="tables",
    )(first, coords)


def kernel(white_ref, right, factor_ref, slow_hbm, out_ref, left, wide, power, slow_ref, slow_in):
    sources, bins, rows, width = white_ref.shape
    segs = rows // 2
    half = grid_size // 4
    step = math.gcd(width, 2 * lane)
    norm = 1.0 / (sources * width * segs)
    slow_copy = pltpu.make_async_copy(slow_hbm, slow_ref, slow_in)
    slow_copy.start()
    def finish(f, total):
        def square(p, q):
            re = p[:, :2 * grid_size] + q[:, 2 * grid_size:]
            im = q[:, :2 * grid_size] - p[:, 2 * grid_size:]
            return re * re + im * im

        plus, minus = 0.0, 0.0
        for g in range(segs):
            rc, rs = (total[2 * half * g + half * i:][:half] for i in (0, 1))
            ic, im = (total[2 * half * (segs + g) + half * i:][:half] for i in (0, 1))
            plus += square(rc + im, ic - rs)
            minus += square(rc - im, ic + rs)
        power[pl.ds(f * 2 * half, half), :] = plus
        power[pl.ds(f * 2 * half + half, half), :] = minus

    def build(f, src):
        for t in range(width // step):
            at = pl.ds(src * width + t * step, step)
            wide[f, :, at] = white_ref[src, f, :, pl.ds(t * step, step)].astype(jnp.float32)
            cos, sin = factor_ref[f, :half, at], factor_ref[f, half:, at]
            for r in range(rows):
                value = jnp.broadcast_to(wide[f, r:r + 1, at], (half, step)).astype(jnp.bfloat16)
                left[f, pl.ds(2 * half * r, half), at] = cos * value
                left[f, pl.ds(2 * half * r + half, half), at] = sin * value

    for f in range(0, bins, 2):
        both = range(f, min(f + 2, bins))
        totals = [0.0] * len(both)
        for src in range(sources):
            for i in both:
                build(i, src)
            at = pl.ds(src * width, width)
            for i in both:
                totals[i - f] += lax.dot_general(
                    left[i, :, at], right[i, :, at], (((1,), (1,)), ((), ())), preferred_element_type=jnp.float32
                )
        for i in both:
            finish(i, totals[i - f])
    slow_copy.wait()
    values = power[...] * norm
    high = values.astype(jnp.bfloat16)
    low = (values - high.astype(jnp.float32)).astype(jnp.bfloat16)
    pair = jnp.concatenate([high, low], 1)
    dests, _, beams = out_ref.shape
    for d in range(dests):
        at = pl.ds(d * beams, beams)
        east = slow_ref[0:1, at]
        north = slow_ref[1:2, at] - grid_low
        column = (east & 1) * grid_size + north
        pick = lax.broadcasted_iota(jnp.int32, (2 * grid_size, beams), 0) == column
        pick = jnp.where(pick, 1.0, 0.0).astype(jnp.bfloat16)
        found = jnp.dot(pair, jnp.concatenate([pick, pick], 0), preferred_element_type=jnp.float32)
        east = jnp.where(east >= 0, east >> 1, half - 1 - (east >> 1))
        row = lax.broadcasted_iota(jnp.int32, (2 * half, beams), 0) == east
        for f in range(bins):
            part = jnp.where(row, found[f * 2 * half:(f + 1) * 2 * half], 0.0)
            out_ref[d, pl.ds(f, 1), :] = jnp.sum(part, axis=0, keepdims=True)


def beam_grid(white, right, factor, slowness, dests):
    sources, bins, rows, width = white.shape
    stations = sources * width
    beams = slowness.shape[1] // dests
    vmem = pl.BlockSpec(memory_space=pltpu.VMEM)
    hbm = pl.BlockSpec(memory_space=pltpu.HBM)
    pin = pltpu.with_memory_space_constraint
    return pl.pallas_call(
        kernel,
        out_shape=jax.ShapeDtypeStruct((dests, bins, beams), jnp.float32),
        in_specs=[vmem, vmem, vmem, hbm],
        out_specs=vmem,
        scratch_shapes=[
            pltpu.VMEM((bins, grid_size // 2 * rows, stations), jnp.bfloat16),
            pltpu.VMEM((bins, rows, stations), jnp.float32),
            pltpu.VMEM((bins * grid_size // 2, 2 * grid_size), jnp.float32),
            pltpu.VMEM(slowness.shape, jnp.int32),
            pltpu.SemaphoreType.DMA,
        ],
        compiler_params=pltpu.CompilerParams(vmem_limit_bytes=vmem_limit),
        cost_estimate=pl.CostEstimate(flops=bins * stations * 4096, bytes_accessed=bins * stations * 576, transcendentals=0),
        name="beam_grid",
    )(white, right, factor, pin(slowness, pltpu.HBM))


def local(spectra, coords, slowness):
    bins_dev = spectra.shape[1]
    seg_count = spectra.shape[2]
    width = spectra.shape[3]
    peers = lax.axis_size("sta")
    groups = math.gcd(bins_dev, peers)
    copies = peers // groups
    bins_own = bins_dev // groups
    values = spectra.astype(jnp.float32)
    local_sq = jnp.sum(values * values, axis=(0, 1))
    total_bins = bins_dev * lax.axis_size("bins")
    rows = lax.axis_size("bins")
    totals = local_sq
    for shift in range(1, rows):
        totals += lax.ppermute(local_sq, "bins", [(i, (i + shift) % rows) for i in range(rows)])
    scale = jnp.sqrt(totals / (2 * total_bins) + epsilon)
    whitened = (values / scale).astype(jnp.bfloat16)
    parts = jnp.transpose(whitened.reshape(2, groups, bins_own, seg_count, width), (1, 2, 0, 3, 4))
    parts = parts.reshape(groups, bins_own, 2 * seg_count, width)
    if copies > 1:
        parts = jnp.repeat(parts, copies, axis=0)
    group = lax.axis_index("sta") // copies
    first = lax.axis_index("bins") * bins_dev + group * bins_own + 1
    right, factor = tables(first.reshape(1).astype(jnp.int32), coords, bins_own)
    parts, right, factor = lax.optimization_barrier((parts, right, factor))
    white = lax.all_to_all(parts, "sta", 0, 0, tiled=True)
    powers = beam_grid(white, right, factor, slowness, peers)
    powers = lax.all_to_all(powers, "sta", 0, 0, tiled=True)
    return powers[::copies].reshape(bins_dev, -1)


def solution(mesh):
    in_specs = (P(None, "bins", None, "sta"), P(), P())
    out_specs = P("bins", "sta")
    return jax.shard_map(local, mesh=mesh, in_specs=in_specs, out_specs=out_specs, check_vma=False)
```

```python
import math

import jax
import jax.numpy as jnp
from jax import lax
from jax.experimental import pallas as pl
from jax.experimental.pallas import tpu as pltpu
from jax.sharding import PartitionSpec as P


phase_modulus = 1048576
epsilon = 1e-06
grid_half = 32
lefts = grid_half // 4
lane = 128
vmem_limit = 32 * 1024 * 1024


def cos_sin(index):
    quarter = phase_modulus // 2
    shift = quarter.bit_length() - 1
    turn = (index + quarter // 2) >> shift
    rest = index - (turn << shift)
    x = rest.astype(jnp.float32) * (math.pi / phase_modulus)
    y = x * x
    s = x + x * y * (-1.6666654611e-1 + y * (8.3321608736e-3 + y * -1.9515295891e-4))
    c = 1 - 0.5 * y + y * y * (4.166664568298827e-2 + y * (-1.388731625493765e-3 + y * 2.443315711809948e-5))
    odd = (turn & 1) == 1
    cos = jnp.where(odd, s, c)
    sin = jnp.where(odd, c, s)
    cos = jnp.where(((turn + 1) & 2) == 2, -cos, cos)
    sin = jnp.where((turn & 2) == 2, -sin, sin)
    return cos, sin


def sums_kernel(spectra_hbm, coords_hbm, slow_hbm, sums_ref, spectra_ref, coords_ref, slow_ref, arrived, small):
    bins = spectra_ref.shape[1]
    piece = math.gcd(bins, 8)
    copies = []
    for i in range(bins // piece):
        at = (slice(None), pl.ds(i * piece, piece))
        copies.append(pltpu.make_async_copy(spectra_hbm.at[at], spectra_ref.at[at], arrived.at[i]))
    copies.append(pltpu.make_async_copy(coords_hbm, coords_ref, small.at[0]))
    copies.append(pltpu.make_async_copy(slow_hbm, slow_ref, small.at[1]))
    for copy in copies:
        copy.start()
    total = 0.0
    for i in range(bins // piece):
        copies[i].wait()
        for f in range(i * piece, (i + 1) * piece):
            for c in range(2):
                values = spectra_ref[c, f].astype(jnp.float32)
                total += values * values
    sums_ref[...] = total
    for copy in copies[bins // piece:]:
        copy.wait()


def sums(spectra, coords, slowness):
    hbm = pl.BlockSpec(memory_space=pltpu.HBM)
    vmem = pl.BlockSpec(memory_space=pltpu.VMEM)
    return pl.pallas_call(
        sums_kernel,
        out_shape=(
            jax.ShapeDtypeStruct(spectra.shape[2:], jnp.float32),
            jax.ShapeDtypeStruct(spectra.shape, spectra.dtype),
            jax.ShapeDtypeStruct(coords.shape, coords.dtype),
            jax.ShapeDtypeStruct(slowness.shape, slowness.dtype),
        ),
        in_specs=[hbm] * 3,
        out_specs=(vmem,) * 4,
        scratch_shapes=[
            pltpu.SemaphoreType.DMA((spectra.shape[1] // math.gcd(spectra.shape[1], 8),)),
            pltpu.SemaphoreType.DMA((2,)),
        ],
        compiler_params=pltpu.CompilerParams(vmem_limit_bytes=vmem_limit),
        cost_estimate=pl.CostEstimate(flops=2 * spectra.size, bytes_accessed=2 * spectra.size, transcendentals=0),
        name="sums",
    )(*(pltpu.with_memory_space_constraint(a, pltpu.HBM) for a in (spectra, coords, slowness)))


def tables_kernel(groups, coords_ref, right_ref, factor_ref, turn_ref):
    bins, columns, stations = right_ref.shape
    _, bins_dev, width = turn_ref.shape
    own = lax.axis_index("sta")
    row_first = lax.axis_index("bins") * bins_dev + 1
    first = row_first + own // (lax.axis_size("sta") // groups) * bins
    mine = pl.ds(pl.multiple_of(own * width, lane), width)
    both = coords_ref[0:1, mine] + coords_ref[1:2, mine]
    piece = math.gcd(bins_dev, 8)
    for i in range(0, bins_dev, piece):
        number = row_first + i + lax.broadcasted_iota(jnp.int32, (piece, width), 0)
        cos, sin = cos_sin(number * both)
        turn_ref[0, pl.ds(i, piece), :] = cos
        turn_ref[1, pl.ds(i, piece), :] = sin

    step = math.gcd(stations, 2 * lane)
    blocks = stations // step
    sub = lax.broadcasted_iota(jnp.int32, (8, step), 0)

    @pl.loop(0, bins * blocks)
    def _(item):
        f = item // blocks
        at = pl.ds(pl.multiple_of(lax.rem(item, blocks) * step, step), step)
        number = first + f
        east = jnp.broadcast_to(coords_ref[0:1, at], (8, step)) * number
        north = jnp.broadcast_to(coords_ref[1:2, at], (8, step)) * number
        factor_ref[f, :, at] = jnp.concatenate(cos_sin(east * (8 * sub + 4)), 0).astype(jnp.bfloat16)
        twice = 2 * cos_sin(16 * north)[0]
        c2, s2 = cos_sin(2 * east)
        start = [cos_sin(east + north * (2 * sub + odd)) for odd in (1 - 2 * grid_half, 17 - 2 * grid_half)]
        turned = [(c * c2 - s * s2, s * c2 + c * s2) for c, s in start]
        for d, (one, two) in enumerate((start, turned)):
            for i in range(0, 2 * grid_half, 16):
                for part in range(2):
                    rows = pl.ds((2 * part + d) * 2 * grid_half + i, 16)
                    right_ref[f, rows, at] = jnp.concatenate([one[part], two[part]], 0).astype(jnp.bfloat16)
                one = tuple(twice * b - a for a, b in zip(one, two))
                two = tuple(twice * b - a for a, b in zip(two, one))


def tables(coords, bins, groups, bins_dev, width):
    stations = coords.shape[1]
    vmem = pl.BlockSpec(memory_space=pltpu.VMEM)
    return pl.pallas_call(
        lambda *refs: tables_kernel(groups, *refs),
        out_shape=(
            jax.ShapeDtypeStruct((bins, 8 * grid_half, stations), jnp.bfloat16),
            jax.ShapeDtypeStruct((bins, 2 * lefts, stations), jnp.bfloat16),
            jax.ShapeDtypeStruct((2, bins_dev, width), jnp.float32),
        ),
        in_specs=[vmem],
        out_specs=(vmem,) * 3,
        compiler_params=pltpu.CompilerParams(vmem_limit_bytes=vmem_limit),
        cost_estimate=pl.CostEstimate(flops=bins * stations * 4096, bytes_accessed=bins * stations * 576, transcendentals=0),
        name="tables",
    )(coords)


def whiten_kernel(total_bins, spectra_ref, turn_ref, *refs):
    *sums_refs, out_ref = refs
    groups, bins, rows, width = out_ref.shape
    total = sum(ref[...] for ref in sums_refs)
    inverse = 1.0 / jnp.sqrt(total / (2 * total_bins) + epsilon)
    for i in range(groups * bins):
        wr = spectra_ref[0, i].astype(jnp.float32) * inverse
        wi = spectra_ref[1, i].astype(jnp.float32) * inverse
        cos, sin = turn_ref[0, i:i + 1, :], turn_ref[1, i:i + 1, :]
        both = jnp.concatenate([wr * cos - wi * sin, wi * cos + wr * sin], 0)
        out_ref[i // bins, i % bins] = both.astype(jnp.bfloat16)


def whiten(spectra, turn, partial, total_bins, groups):
    _, bins_dev, segs, width = spectra.shape
    vmem = pl.BlockSpec(memory_space=pltpu.VMEM)
    return pl.pallas_call(
        lambda *refs: whiten_kernel(total_bins, *refs),
        out_shape=jax.ShapeDtypeStruct((groups, bins_dev // groups, 2 * segs, width), jnp.bfloat16),
        in_specs=[vmem] * (2 + len(partial)),
        out_specs=vmem,
        compiler_params=pltpu.CompilerParams(vmem_limit_bytes=vmem_limit),
        cost_estimate=pl.CostEstimate(flops=8 * spectra.size, bytes_accessed=4 * spectra.size, transcendentals=0),
        name="whiten",
    )(spectra, turn, *partial)


def grid_kernel(white_ref, right_ref, factor_ref, slow_ref, out_ref, left, power):
    sources, bins, rows, width = white_ref.shape
    segs = rows // 2
    basis = 2 * lefts
    step = math.gcd(width, 2 * lane)
    norm = 1.0 / (sources * width * segs)
    columns = 4 * grid_half

    def build(f, src):
        for t in range(width // step):
            at = pl.ds(src * width + t * step, step)
            white = white_ref[src, f, :, pl.ds(t * step, step)].astype(jnp.float32)
            factor = factor_ref[f, :, at]
            for r in range(rows):
                value = jnp.broadcast_to(white[r:r + 1], (basis, step)).astype(jnp.bfloat16)
                left[f, pl.ds(basis * r, basis), at] = factor * value

    def finish(f, total):
        found = [0.0] * 4
        for g in range(segs):
            real = total[basis * g:basis * (g + 1)]
            imag = total[basis * (segs + g):basis * (segs + g + 1)]
            rcc, rcs = real[:lefts, :columns], real[:lefts, columns:]
            rsc, rss = real[lefts:, :columns], real[lefts:, columns:]
            icc, ics = imag[:lefts, :columns], imag[:lefts, columns:]
            isc, iss = imag[lefts:, :columns], imag[lefts:, columns:]
            same = (rcc - rss, isc + ics, icc - iss, rsc + rcs)
            mixed = (rcc + rss, isc - ics, icc + iss, rsc - rcs)
            for q, (a, b, c, d) in ((0, same), (2, mixed)):
                found[q] += (a + b) * (a + b) + (c - d) * (c - d)
                found[q + 1] += (a - b) * (a - b) + (c + d) * (c + d)
        for q in range(4):
            power[pl.ds((4 * f + q) * lefts, lefts), :] = found[q] * norm

    for f in range(0, bins, 2):
        both = range(f, min(f + 2, bins))
        totals = [0.0] * len(both)
        for src in range(sources):
            for i in both:
                build(i, src)
            at = pl.ds(src * width, width)
            for i in both:
                totals[i - f] += lax.dot_general(
                    left[i, :, at], right_ref[i, :, at], (((1,), (1,)), ((), ())), preferred_element_type=jnp.float32
                )
        for i in both:
            finish(i, totals[i - f])

    values = power[...]
    high = values.astype(jnp.bfloat16)
    low = (values - high.astype(jnp.float32)).astype(jnp.bfloat16)
    pair = jnp.concatenate([high, low], 1)
    dests, _, beams = out_ref.shape
    for d in range(dests):
        at = pl.ds(d * beams, beams)
        east = 2 * slow_ref[0:1, at] + 1
        north = slow_ref[1:2, at]
        size = jnp.abs(east)
        place = (size & 7) >> 1
        positive = east > 0
        same = positive == (place >= 2)
        column = jnp.where(same, north + grid_half, grid_half - 1 - north)
        column += jnp.where((place == 1) | (place == 2), 0, 2 * grid_half)
        sign = jnp.where(place >= 2, jnp.where(positive, 0, 1), jnp.where(positive, 2, 3))
        wanted = sign * lefts + (size >> 3)
        pick = lax.broadcasted_iota(jnp.int32, (columns, beams), 0) == column
        pick = jnp.where(pick, 1.0, 0.0).astype(jnp.bfloat16)
        found = jnp.dot(pair, jnp.concatenate([pick, pick], 0), preferred_element_type=jnp.float32)
        row = lax.broadcasted_iota(jnp.int32, (4 * lefts, beams), 0) == wanted
        for f in range(bins):
            part = jnp.where(row, found[f * 4 * lefts:(f + 1) * 4 * lefts], 0.0)
            out_ref[d, pl.ds(f, 1), :] = jnp.sum(part, axis=0, keepdims=True)


def beam_grid(white, right, factor, slowness, dests):
    sources, bins, rows, width = white.shape
    stations = sources * width
    beams = slowness.shape[1] // dests
    vmem = pl.BlockSpec(memory_space=pltpu.VMEM)
    return pl.pallas_call(
        grid_kernel,
        out_shape=jax.ShapeDtypeStruct((dests, bins, beams), jnp.float32),
        in_specs=[vmem] * 4,
        out_specs=vmem,
        scratch_shapes=[
            pltpu.VMEM((bins, 2 * lefts * rows, stations), jnp.bfloat16),
            pltpu.VMEM((bins * 4 * lefts, 4 * grid_half), jnp.float32),
        ],
        compiler_params=pltpu.CompilerParams(vmem_limit_bytes=vmem_limit),
        cost_estimate=pl.CostEstimate(flops=bins * stations * 4096, bytes_accessed=bins * stations * 576, transcendentals=0),
        name="beam_grid",
    )(white, right, factor, slowness)


def local(spectra, coords, slowness):
    _, bins_dev, _, width = spectra.shape
    peers = lax.axis_size("sta")
    rows = lax.axis_size("bins")
    groups = math.gcd(bins_dev, peers)
    copies = peers // groups
    bins_own = bins_dev // groups
    local_sq, spectra, coords, slowness = sums(spectra, coords, slowness)
    partial = [local_sq]
    for shift in range(1, rows):
        partial.append(lax.ppermute(local_sq, "bins", [(i, (i + shift) % rows) for i in range(rows)]))
    right, factor, turn = tables(coords, bins_own, groups, bins_dev, width)
    parts = whiten(spectra, turn, partial, bins_dev * rows, groups)
    if copies > 1:
        parts = jnp.repeat(parts, copies, axis=0)
    white = lax.all_to_all(parts, "sta", 0, 0, tiled=True)
    powers = beam_grid(white, right, factor, slowness, peers)
    powers = lax.all_to_all(powers, "sta", 0, 0, tiled=True)
    return powers[::copies].reshape(bins_dev, -1)


def solution(mesh):
    in_specs = (P(None, "bins", None, "sta"), P(), P())
    out_specs = P("bins", "sta")
    return jax.shard_map(local, mesh=mesh, in_specs=in_specs, out_specs=out_specs, check_vma=False)
```

```python
import math

import jax
import jax.numpy as jnp
from jax import lax
from jax.experimental import pallas as pl
from jax.experimental.pallas import tpu as pltpu
from jax.sharding import PartitionSpec as P


phase_modulus = 1048576
epsilon = 1e-06
grid_half = 32
lefts = grid_half // 4
lane = 128
vmem_limit = 32 * 1024 * 1024


def cos_sin(index):
    shift = 33 - (2 * phase_modulus).bit_length()
    rest = (index << shift) >> shift
    x = rest.astype(jnp.float32) * (math.pi / (4 * phase_modulus))
    y = x * x
    sin = x + x * y * (-1.6666654611e-1 + y * (8.3321608736e-3 + y * -1.9515295891e-4))
    cos = 1 - 0.5 * y + y * y * (4.166664568298827e-2 + y * (-1.388731625493765e-3 + y * 2.443315711809948e-5))
    for _ in range(2):
        twice = sin + sin
        cos, sin = 1 - twice * sin, twice * cos
    return cos, sin


def rotate(one, two):
    return one[0] * two[0] - one[1] * two[1], one[1] * two[0] + one[0] * two[1]


def sums_kernel(spectra_hbm, coords_hbm, slow_hbm, sums_ref, spectra_ref, coords_ref, slow_ref, arrived, small):
    bins = spectra_ref.shape[1]
    piece = math.gcd(bins, 8)
    copies = []
    for i in range(bins // piece):
        at = (slice(None), pl.ds(i * piece, piece))
        copies.append(pltpu.make_async_copy(spectra_hbm.at[at], spectra_ref.at[at], arrived.at[i]))
    copies.append(pltpu.make_async_copy(coords_hbm, coords_ref, small.at[0]))
    copies.append(pltpu.make_async_copy(slow_hbm, slow_ref, small.at[1]))
    for copy in copies:
        copy.start()
    total = 0.0
    for i in range(bins // piece):
        copies[i].wait()
        for f in range(i * piece, (i + 1) * piece):
            for c in range(2):
                values = spectra_ref[c, f].astype(jnp.float32)
                total += values * values
    sums_ref[...] = total
    for copy in copies[bins // piece:]:
        copy.wait()


def sums(spectra, coords, slowness):
    hbm = pl.BlockSpec(memory_space=pltpu.HBM)
    vmem = pl.BlockSpec(memory_space=pltpu.VMEM)
    return pl.pallas_call(
        sums_kernel,
        out_shape=(
            jax.ShapeDtypeStruct(spectra.shape[2:], jnp.float32),
            jax.ShapeDtypeStruct(spectra.shape, spectra.dtype),
            jax.ShapeDtypeStruct(coords.shape, coords.dtype),
            jax.ShapeDtypeStruct(slowness.shape, slowness.dtype),
        ),
        in_specs=[hbm] * 3,
        out_specs=(vmem,) * 4,
        scratch_shapes=[
            pltpu.SemaphoreType.DMA((spectra.shape[1] // math.gcd(spectra.shape[1], 8),)),
            pltpu.SemaphoreType.DMA((2,)),
        ],
        compiler_params=pltpu.CompilerParams(vmem_limit_bytes=vmem_limit),
        cost_estimate=pl.CostEstimate(flops=2 * spectra.size, bytes_accessed=2 * spectra.size, transcendentals=0),
        name="sums",
    )(*(pltpu.with_memory_space_constraint(a, pltpu.HBM) for a in (spectra, coords, slowness)))


def tables_kernel(groups, coords_ref, slow_ref, right_ref, factor_ref, turn_ref, pick_ref, wanted_ref, rows_ref):
    bins, columns, stations = right_ref.shape
    _, bins_dev, width = turn_ref.shape
    own = lax.axis_index("sta")
    row_first = lax.axis_index("bins") * bins_dev + 1
    first = row_first + own // (lax.axis_size("sta") // groups) * bins
    mine = pl.ds(pl.multiple_of(own * width, lane), width)
    both = coords_ref[0:1, mine] + coords_ref[1:2, mine]
    piece = math.gcd(bins_dev, 8)
    for i in range(0, bins_dev, piece):
        number = row_first + i + lax.broadcasted_iota(jnp.int32, (piece, width), 0)
        cos, sin = cos_sin(number * both)
        turn_ref[0, pl.ds(i, piece), :] = cos
        turn_ref[1, pl.ds(i, piece), :] = sin

    beams = slow_ref.shape[1]
    columns = 4 * grid_half
    piece = math.gcd(beams, 2 * lane)
    for i in range(0, beams, piece):
        at = pl.ds(i, piece)
        east = 2 * slow_ref[0:1, at] + 1
        north = slow_ref[1:2, at]
        size = jnp.abs(east)
        place = (size & 7) >> 1
        positive = east > 0
        same = positive == (place >= 2)
        column = jnp.where(same, north + grid_half, grid_half - 1 - north)
        column += jnp.where((place == 1) | (place == 2), 0, 2 * grid_half)
        sign = jnp.where(place >= 2, jnp.where(positive, 0, 1), jnp.where(positive, 2, 3))
        wanted_ref[0:1, at] = sign * lefts + (size >> 3)
        pick = lax.broadcasted_iota(jnp.int32, (columns, piece), 0) == column
        pick_ref[:, at] = jnp.where(pick, 1.0, 0.0).astype(jnp.bfloat16)

    step = math.gcd(stations, 2 * lane)
    sub = lax.broadcasted_iota(jnp.int32, (8, step), 0)
    odd = (sub & 1) == 1

    @pl.loop(0, stations // step)
    def _(block):
        at = pl.ds(pl.multiple_of(block * step, step), step)
        east = jnp.broadcast_to(coords_ref[0:1, at], (8, step))
        north = jnp.broadcast_to(coords_ref[1:2, at], (8, step))
        for i in range(0, 2 * bins, 8):
            index = jnp.where(odd, 2 * east, 16 * north) * (first + i // 2 + (sub >> 1))
            for part, values in enumerate(cos_sin(index)):
                rows_ref[part, pl.ds(i, 8), :] = values
        start_unit = east + north * (2 * sub + (1 - 2 * grid_half))
        factor_unit = east * (8 * sub + 4)
        start, factor = cos_sin(start_unit * first), cos_sin(factor_unit * first)
        if bins > 1:
            start_unit, factor_unit = cos_sin(start_unit), cos_sin(factor_unit)
        for f in range(bins):
            if f > 0:
                start, factor = rotate(start, start_unit), rotate(factor, factor_unit)
            sixteen, two_east = (
                tuple(jnp.broadcast_to(rows_ref[part, r:r + 1, :], (8, step)) for part in range(2))
                for r in (2 * f, 2 * f + 1)
            )
            factor_ref[f, :, at] = jnp.concatenate(factor, 0)
            twice = 2 * sixteen[0]
            second = rotate(start, sixteen)
            for d, (one, two) in enumerate(((start, second), (rotate(start, two_east), rotate(second, two_east)))):
                for i in range(0, 2 * grid_half, 16):
                    for part in range(2):
                        rows = pl.ds((2 * part + d) * 2 * grid_half + i, 16)
                        right_ref[f, rows, at] = jnp.concatenate([one[part], two[part]], 0).astype(jnp.bfloat16)
                    one = tuple(twice * b - a for a, b in zip(one, two))
                    two = tuple(twice * b - a for a, b in zip(two, one))


def tables(coords, slowness, bins, groups, bins_dev, width):
    stations = coords.shape[1]
    vmem = pl.BlockSpec(memory_space=pltpu.VMEM)
    return pl.pallas_call(
        lambda *refs: tables_kernel(groups, *refs),
        out_shape=(
            jax.ShapeDtypeStruct((bins, 8 * grid_half, stations), jnp.bfloat16),
            jax.ShapeDtypeStruct((bins, 2 * lefts, stations), jnp.float32),
            jax.ShapeDtypeStruct((2, bins_dev, width), jnp.float32),
            jax.ShapeDtypeStruct((4 * grid_half, slowness.shape[1]), jnp.bfloat16),
            jax.ShapeDtypeStruct((1, slowness.shape[1]), jnp.int32),
        ),
        in_specs=[vmem] * 2,
        out_specs=(vmem,) * 5,
        scratch_shapes=[pltpu.VMEM((2, 8 * pl.cdiv(bins, 4), math.gcd(stations, 2 * lane)), jnp.float32)],
        compiler_params=pltpu.CompilerParams(vmem_limit_bytes=vmem_limit),
        cost_estimate=pl.CostEstimate(flops=bins * stations * 4096, bytes_accessed=bins * stations * 576, transcendentals=0),
        name="tables",
    )(coords, slowness)


def whiten_kernel(total_bins, spectra_ref, turn_ref, *refs):
    *sums_refs, out_ref = refs
    groups, bins, rows, width = out_ref.shape
    total = sum(ref[...] for ref in sums_refs)
    inverse = 1.0 / jnp.sqrt(total / (2 * total_bins) + epsilon)
    for i in range(groups * bins):
        wr = spectra_ref[0, i].astype(jnp.float32) * inverse
        wi = spectra_ref[1, i].astype(jnp.float32) * inverse
        cos, sin = turn_ref[0, i:i + 1, :], turn_ref[1, i:i + 1, :]
        both = jnp.concatenate([wr * cos - wi * sin, wi * cos + wr * sin], 0)
        out_ref[i // bins, i % bins] = both.astype(jnp.bfloat16)


def whiten(spectra, turn, partial, total_bins, groups):
    _, bins_dev, segs, width = spectra.shape
    vmem = pl.BlockSpec(memory_space=pltpu.VMEM)
    return pl.pallas_call(
        lambda *refs: whiten_kernel(total_bins, *refs),
        out_shape=jax.ShapeDtypeStruct((groups, bins_dev // groups, 2 * segs, width), jnp.bfloat16),
        in_specs=[vmem] * (2 + len(partial)),
        out_specs=vmem,
        compiler_params=pltpu.CompilerParams(vmem_limit_bytes=vmem_limit),
        cost_estimate=pl.CostEstimate(flops=8 * spectra.size, bytes_accessed=4 * spectra.size, transcendentals=0),
        name="whiten",
    )(spectra, turn, *partial)


def grid_kernel(white_ref, right_ref, factor_ref, pick_ref, wanted_ref, out_ref, left, power):
    sources, bins, rows, width = white_ref.shape
    segs = rows // 2
    basis = 2 * lefts
    step = math.gcd(width, 2 * lane)
    norm = 1.0 / (sources * width * segs)
    columns = 4 * grid_half

    def build(f, src):
        for t in range(width // step):
            at = pl.ds(src * width + t * step, step)
            white = white_ref[src, f, :, pl.ds(t * step, step)].astype(jnp.float32)
            factor = factor_ref[f, :, at].astype(jnp.float32)
            for r in range(rows):
                value = jnp.broadcast_to(white[r:r + 1], (basis, step))
                left[f, pl.ds(basis * r, basis), at] = (factor * value).astype(jnp.bfloat16)

    def finish(f, total):
        found = [0.0] * 4
        for g in range(segs):
            real = total[basis * g:basis * (g + 1)]
            imag = total[basis * (segs + g):basis * (segs + g + 1)]
            rcc, rcs = real[:lefts, :columns], real[:lefts, columns:]
            rsc, rss = real[lefts:, :columns], real[lefts:, columns:]
            icc, ics = imag[:lefts, :columns], imag[:lefts, columns:]
            isc, iss = imag[lefts:, :columns], imag[lefts:, columns:]
            same = (rcc - rss, isc + ics, icc - iss, rsc + rcs)
            mixed = (rcc + rss, isc - ics, icc + iss, rsc - rcs)
            for q, (a, b, c, d) in ((0, same), (2, mixed)):
                found[q] += (a + b) * (a + b) + (c - d) * (c - d)
                found[q + 1] += (a - b) * (a - b) + (c + d) * (c + d)
        for q in range(4):
            power[pl.ds((4 * f + q) * lefts, lefts), :] = found[q] * norm

    dests, _, beams = out_ref.shape

    for f in range(0, bins, 2):
        both = range(f, min(f + 2, bins))
        totals = [0.0] * len(both)
        for src in range(sources):
            for i in both:
                build(i, src)
            at = pl.ds(src * width, width)
            for i in both:
                totals[i - f] += lax.dot_general(
                    left[i, :, at], right_ref[i, :, at], (((1,), (1,)), ((), ())), preferred_element_type=jnp.float32
                )
        for i in both:
            finish(i, totals[i - f])

    values = power[...]
    high = values.astype(jnp.bfloat16)
    low = (values - high.astype(jnp.float32)).astype(jnp.bfloat16)
    pair = jnp.concatenate([high, low], 1)
    for d in range(dests):
        at = pl.ds(d * beams, beams)
        pick = pick_ref[:, at]
        found = jnp.dot(pair, jnp.concatenate([pick, pick], 0), preferred_element_type=jnp.float32)
        row = lax.broadcasted_iota(jnp.int32, (4 * lefts, beams), 0) == wanted_ref[0:1, at]
        for f in range(bins):
            part = jnp.where(row, found[f * 4 * lefts:(f + 1) * 4 * lefts], 0.0)
            out_ref[d, pl.ds(f, 1), :] = jnp.sum(part, axis=0, keepdims=True)


def beam_grid(white, right, factor, pick, wanted, dests):
    sources, bins, rows, width = white.shape
    stations = sources * width
    beams = pick.shape[1] // dests
    vmem = pl.BlockSpec(memory_space=pltpu.VMEM)
    return pl.pallas_call(
        grid_kernel,
        out_shape=jax.ShapeDtypeStruct((dests, bins, beams), jnp.float32),
        in_specs=[vmem] * 5,
        out_specs=vmem,
        scratch_shapes=[
            pltpu.VMEM((bins, 2 * lefts * rows, stations), jnp.bfloat16),
            pltpu.VMEM((bins * 4 * lefts, 4 * grid_half), jnp.float32),
        ],
        compiler_params=pltpu.CompilerParams(vmem_limit_bytes=vmem_limit),
        cost_estimate=pl.CostEstimate(flops=bins * stations * 4096, bytes_accessed=bins * stations * 576, transcendentals=0),
        name="beam_grid",
    )(white, right, factor, pick, wanted)


def local(spectra, coords, slowness):
    _, bins_dev, _, width = spectra.shape
    peers = lax.axis_size("sta")
    rows = lax.axis_size("bins")
    groups = math.gcd(bins_dev, peers)
    copies = peers // groups
    bins_own = bins_dev // groups
    local_sq, spectra, coords, slowness = sums(spectra, coords, slowness)
    partial = [local_sq]
    for shift in range(1, rows):
        partial.append(lax.ppermute(local_sq, "bins", [(i, (i + shift) % rows) for i in range(rows)]))
    right, factor, turn, pick, wanted = tables(coords, slowness, bins_own, groups, bins_dev, width)
    parts = whiten(spectra, turn, partial, bins_dev * rows, groups)
    if copies > 1:
        parts = jnp.repeat(parts, copies, axis=0)
    white = lax.all_to_all(parts, "sta", 0, 0, tiled=True)
    powers = beam_grid(white, right, factor, pick, wanted, peers)
    powers = lax.all_to_all(powers, "sta", 0, 0, tiled=True)
    return powers[::copies].reshape(bins_dev, -1)


def solution(mesh):
    in_specs = (P(None, "bins", None, "sta"), P(), P())
    out_specs = P("bins", "sta")
    return jax.shard_map(local, mesh=mesh, in_specs=in_specs, out_specs=out_specs, check_vma=False)
```

```python
import math

import jax
import jax.numpy as jnp
from jax import lax
from jax.experimental import pallas as pl
from jax.experimental.pallas import tpu as pltpu
from jax.sharding import PartitionSpec as P


phase_modulus = 1048576
epsilon = 1e-06
grid_half = 32
lefts = grid_half // 4
lane = 128
vmem_limit = 32 * 1024 * 1024


def cos_sin(index):
    shift = 33 - (2 * phase_modulus).bit_length()
    rest = (index << shift) >> shift
    x = rest.astype(jnp.float32) * (math.pi / (4 * phase_modulus))
    y = x * x
    sin = x + x * y * (-1.6666654611e-1 + y * (8.3321608736e-3 + y * -1.9515295891e-4))
    cos = 1 - 0.5 * y + y * y * (4.166664568298827e-2 + y * (-1.388731625493765e-3 + y * 2.443315711809948e-5))
    for _ in range(2):
        twice = sin + sin
        cos, sin = 1 - twice * sin, twice * cos
    return cos, sin


def rotate(one, two):
    return one[0] * two[0] - one[1] * two[1], one[1] * two[0] + one[0] * two[1]


def sums_kernel(
    spectra_hbm, coords_hbm, slow_hbm, sums_ref, spectra_ref, coords_ref, turn_ref, pick_ref, wanted_ref, slow_ref, arrived, small
):
    _, bins, _, width = spectra_ref.shape
    slow_copy = pltpu.make_async_copy(slow_hbm, slow_ref, small.at[0])
    coords_copy = pltpu.make_async_copy(coords_hbm, coords_ref, small.at[1])
    slow_copy.start()
    coords_copy.start()
    piece = math.gcd(bins, 8)
    copies = []
    for i in range(0, bins, piece):
        at = (slice(None), pl.ds(i, piece))
        copies.append(pltpu.make_async_copy(spectra_hbm.at[at], spectra_ref.at[at], arrived.at[i // piece]))
        copies[-1].start()

    slow_copy.wait()
    beams = slow_ref.shape[1]
    columns = 4 * grid_half
    block = math.gcd(beams, 2 * lane)
    for i in range(0, beams, block):
        at = pl.ds(i, block)
        east = 2 * slow_ref[0:1, at] + 1
        north = slow_ref[1:2, at]
        size = jnp.abs(east)
        place = (size & 7) >> 1
        positive = east > 0
        same = positive == (place >= 2)
        column = jnp.where(same, north + grid_half, grid_half - 1 - north)
        column += jnp.where((place == 1) | (place == 2), 0, 2 * grid_half)
        sign = jnp.where(place >= 2, jnp.where(positive, 0, 1), jnp.where(positive, 2, 3))
        wanted_ref[0:1, at] = sign * lefts + (size >> 3)
        pick = lax.broadcasted_iota(jnp.int32, (columns, block), 0) == column
        pick_ref[:, at] = jnp.where(pick, 1.0, 0.0).astype(jnp.bfloat16)

    coords_copy.wait()
    mine = pl.ds(pl.multiple_of(lax.axis_index("sta") * width, lane), width)
    both = coords_ref[0:1, mine] + coords_ref[1:2, mine]
    for i in range(0, bins, piece):
        number = lax.axis_index("bins") * bins + (i + 1) + lax.broadcasted_iota(jnp.int32, (piece, width), 0)
        for part, values in enumerate(cos_sin(number * both)):
            turn_ref[part, pl.ds(i, piece), :] = values

    total = 0.0
    for i in range(0, bins, piece):
        copies[i // piece].wait()
        for f in range(i, i + piece):
            for c in range(2):
                values = spectra_ref[c, f].astype(jnp.float32)
                total += values * values
    sums_ref[...] = total


def sums(spectra, coords, slowness):
    _, bins, segs, width = spectra.shape
    beams = slowness.shape[1]
    hbm = pl.BlockSpec(memory_space=pltpu.HBM)
    vmem = pl.BlockSpec(memory_space=pltpu.VMEM)
    return pl.pallas_call(
        sums_kernel,
        out_shape=(
            jax.ShapeDtypeStruct((segs, width), jnp.float32),
            jax.ShapeDtypeStruct(spectra.shape, spectra.dtype),
            jax.ShapeDtypeStruct(coords.shape, coords.dtype),
            jax.ShapeDtypeStruct((2, bins, width), jnp.float32),
            jax.ShapeDtypeStruct((4 * grid_half, beams), jnp.bfloat16),
            jax.ShapeDtypeStruct((1, beams), jnp.int32),
        ),
        in_specs=[hbm] * 3,
        out_specs=(vmem,) * 6,
        scratch_shapes=[
            pltpu.VMEM(slowness.shape, slowness.dtype),
            pltpu.SemaphoreType.DMA((bins // math.gcd(bins, 8),)),
            pltpu.SemaphoreType.DMA((2,)),
        ],
        compiler_params=pltpu.CompilerParams(vmem_limit_bytes=vmem_limit),
        cost_estimate=pl.CostEstimate(flops=2 * spectra.size, bytes_accessed=2 * spectra.size, transcendentals=0),
        name="sums",
    )(*(pltpu.with_memory_space_constraint(a, pltpu.HBM) for a in (spectra, coords, slowness)))


def tables_kernel(groups, bins_dev, coords_ref, right_ref, factor_ref, rows_ref):
    bins, _, stations = right_ref.shape
    first = lax.axis_index("bins") * bins_dev + 1
    first += lax.axis_index("sta") // (lax.axis_size("sta") // groups) * bins
    step = math.gcd(stations, 2 * lane)
    sub = lax.broadcasted_iota(jnp.int32, (8, step), 0)
    odd = (sub & 1) == 1

    @pl.loop(0, stations // step)
    def _(block):
        at = pl.ds(pl.multiple_of(block * step, step), step)
        east = jnp.broadcast_to(coords_ref[0:1, at], (8, step))
        north = jnp.broadcast_to(coords_ref[1:2, at], (8, step))
        for i in range(0, 2 * bins, 8):
            index = jnp.where(odd, 2 * east, 16 * north) * (first + i // 2 + (sub >> 1))
            for part, values in enumerate(cos_sin(index)):
                rows_ref[part, pl.ds(i, 8), :] = values
        start_unit = east + north * (2 * sub + (1 - 2 * grid_half))
        factor_unit = east * (8 * sub + 4)
        start, factor = cos_sin(start_unit * first), cos_sin(factor_unit * first)
        if bins > 1:
            start_unit, factor_unit = cos_sin(start_unit), cos_sin(factor_unit)
        for f in range(bins):
            if f > 0:
                start, factor = rotate(start, start_unit), rotate(factor, factor_unit)
            sixteen, two_east = (
                tuple(jnp.broadcast_to(rows_ref[part, r:r + 1, :], (8, step)) for part in range(2))
                for r in (2 * f, 2 * f + 1)
            )
            factor_ref[f, :, at] = jnp.concatenate(factor, 0)
            twice = 2 * sixteen[0]
            second = rotate(start, sixteen)
            for d, (one, two) in enumerate(((start, second), (rotate(start, two_east), rotate(second, two_east)))):
                for i in range(0, 2 * grid_half, 16):
                    for part in range(2):
                        rows = pl.ds((2 * part + d) * 2 * grid_half + i, 16)
                        right_ref[f, rows, at] = jnp.concatenate([one[part], two[part]], 0).astype(jnp.bfloat16)
                    one = tuple(twice * b - a for a, b in zip(one, two))
                    two = tuple(twice * b - a for a, b in zip(two, one))


def tables(coords, bins, groups, bins_dev):
    stations = coords.shape[1]
    vmem = pl.BlockSpec(memory_space=pltpu.VMEM)
    return pl.pallas_call(
        lambda *refs: tables_kernel(groups, bins_dev, *refs),
        out_shape=(
            jax.ShapeDtypeStruct((bins, 8 * grid_half, stations), jnp.bfloat16),
            jax.ShapeDtypeStruct((bins, 2 * lefts, stations), jnp.float32),
        ),
        in_specs=[vmem],
        out_specs=(vmem,) * 2,
        scratch_shapes=[pltpu.VMEM((2, 8 * pl.cdiv(bins, 4), math.gcd(stations, 2 * lane)), jnp.float32)],
        compiler_params=pltpu.CompilerParams(vmem_limit_bytes=vmem_limit),
        cost_estimate=pl.CostEstimate(flops=bins * stations * 4096, bytes_accessed=bins * stations * 576, transcendentals=0),
        name="tables",
    )(coords)


def whiten_kernel(total_bins, spectra_ref, turn_ref, *refs):
    *sums_refs, out_ref = refs
    groups, bins, rows, width = out_ref.shape
    total = sum(ref[...] for ref in sums_refs)
    inverse = 1.0 / jnp.sqrt(total / (2 * total_bins) + epsilon)
    for i in range(groups * bins):
        wr = spectra_ref[0, i].astype(jnp.float32) * inverse
        wi = spectra_ref[1, i].astype(jnp.float32) * inverse
        cos, sin = turn_ref[0, i:i + 1, :], turn_ref[1, i:i + 1, :]
        both = jnp.concatenate([wr * cos - wi * sin, wi * cos + wr * sin], 0)
        out_ref[i // bins, i % bins] = both.astype(jnp.bfloat16)


def whiten(spectra, turn, partial, total_bins, groups):
    _, bins_dev, segs, width = spectra.shape
    vmem = pl.BlockSpec(memory_space=pltpu.VMEM)
    return pl.pallas_call(
        lambda *refs: whiten_kernel(total_bins, *refs),
        out_shape=jax.ShapeDtypeStruct((groups, bins_dev // groups, 2 * segs, width), jnp.bfloat16),
        in_specs=[vmem] * (2 + len(partial)),
        out_specs=vmem,
        compiler_params=pltpu.CompilerParams(vmem_limit_bytes=vmem_limit),
        cost_estimate=pl.CostEstimate(flops=8 * spectra.size, bytes_accessed=4 * spectra.size, transcendentals=0),
        name="whiten",
    )(spectra, turn, *partial)


def grid_kernel(white_ref, right_ref, factor_ref, pick_ref, wanted_ref, out_ref, left, power):
    sources, bins, rows, width = white_ref.shape
    segs = rows // 2
    basis = 2 * lefts
    step = math.gcd(width, 2 * lane)
    norm = 1.0 / (sources * width * segs)
    columns = 4 * grid_half

    def build(f, src):
        for t in range(width // step):
            at = pl.ds(src * width + t * step, step)
            white = white_ref[src, f, :, pl.ds(t * step, step)].astype(jnp.float32)
            factor = factor_ref[f, :, at].astype(jnp.float32)
            for r in range(rows):
                value = jnp.broadcast_to(white[r:r + 1], (basis, step))
                left[f, pl.ds(basis * r, basis), at] = (factor * value).astype(jnp.bfloat16)

    def finish(f, total):
        found = [0.0] * 4
        for g in range(segs):
            real = total[basis * g:basis * (g + 1)]
            imag = total[basis * (segs + g):basis * (segs + g + 1)]
            rcc, rcs = real[:lefts, :columns], real[:lefts, columns:]
            rsc, rss = real[lefts:, :columns], real[lefts:, columns:]
            icc, ics = imag[:lefts, :columns], imag[:lefts, columns:]
            isc, iss = imag[lefts:, :columns], imag[lefts:, columns:]
            same = (rcc - rss, isc + ics, icc - iss, rsc + rcs)
            mixed = (rcc + rss, isc - ics, icc + iss, rsc - rcs)
            for q, (a, b, c, d) in ((0, same), (2, mixed)):
                found[q] += (a + b) * (a + b) + (c - d) * (c - d)
                found[q + 1] += (a - b) * (a - b) + (c + d) * (c + d)
        for q in range(4):
            power[pl.ds((4 * f + q) * lefts, lefts), :] = found[q] * norm

    dests, _, beams = out_ref.shape

    for f in range(0, bins, 2):
        both = range(f, min(f + 2, bins))
        totals = [0.0] * len(both)
        for src in range(sources):
            for i in both:
                build(i, src)
            at = pl.ds(src * width, width)
            for i in both:
                totals[i - f] += lax.dot_general(
                    left[i, :, at], right_ref[i, :, at], (((1,), (1,)), ((), ())), preferred_element_type=jnp.float32
                )
        for i in both:
            finish(i, totals[i - f])

    values = power[...]
    high = values.astype(jnp.bfloat16)
    low = (values - high.astype(jnp.float32)).astype(jnp.bfloat16)
    pair = jnp.concatenate([high, low], 1)
    for d in range(dests):
        at = pl.ds(d * beams, beams)
        pick = pick_ref[:, at]
        found = jnp.dot(pair, jnp.concatenate([pick, pick], 0), preferred_element_type=jnp.float32)
        row = lax.broadcasted_iota(jnp.int32, (4 * lefts, beams), 0) == wanted_ref[0:1, at]
        for f in range(bins):
            part = jnp.where(row, found[f * 4 * lefts:(f + 1) * 4 * lefts], 0.0)
            out_ref[d, pl.ds(f, 1), :] = jnp.sum(part, axis=0, keepdims=True)


def beam_grid(white, right, factor, pick, wanted, dests):
    sources, bins, rows, width = white.shape
    stations = sources * width
    beams = pick.shape[1] // dests
    vmem = pl.BlockSpec(memory_space=pltpu.VMEM)
    return pl.pallas_call(
        grid_kernel,
        out_shape=jax.ShapeDtypeStruct((dests, bins, beams), jnp.float32),
        in_specs=[vmem] * 5,
        out_specs=vmem,
        scratch_shapes=[
            pltpu.VMEM((bins, 2 * lefts * rows, stations), jnp.bfloat16),
            pltpu.VMEM((bins * 4 * lefts, 4 * grid_half), jnp.float32),
        ],
        compiler_params=pltpu.CompilerParams(vmem_limit_bytes=vmem_limit),
        cost_estimate=pl.CostEstimate(flops=bins * stations * 4096, bytes_accessed=bins * stations * 576, transcendentals=0),
        name="beam_grid",
    )(white, right, factor, pick, wanted)


def local(spectra, coords, slowness):
    _, bins_dev, _, width = spectra.shape
    peers = lax.axis_size("sta")
    rows = lax.axis_size("bins")
    groups = math.gcd(bins_dev, peers)
    copies = peers // groups
    bins_own = bins_dev // groups
    local_sq, spectra, coords, turn, pick, wanted = sums(spectra, coords, slowness)
    partial = [local_sq]
    for shift in sorted(range(1, rows), key=lambda k: (k != rows // 2, k)):
        partial.append(lax.ppermute(local_sq, "bins", [(i, (i + shift) % rows) for i in range(rows)]))
    right, factor = tables(coords, bins_own, groups, bins_dev)
    parts = whiten(spectra, turn, partial, bins_dev * rows, groups)
    if copies > 1:
        parts = jnp.repeat(parts, copies, axis=0)
    parts, right, factor = lax.optimization_barrier((parts, right, factor))
    white = lax.all_to_all(parts, "sta", 0, 0, tiled=True)
    powers = beam_grid(white, right, factor, pick, wanted, peers)
    powers = lax.all_to_all(powers, "sta", 0, 0, tiled=True)
    return powers[::copies].reshape(bins_dev, -1)


def solution(mesh):
    in_specs = (P(None, "bins", None, "sta"), P(), P())
    out_specs = P("bins", "sta")
    return jax.shard_map(local, mesh=mesh, in_specs=in_specs, out_specs=out_specs, check_vma=False)
```

```python
import math

import jax
import jax.numpy as jnp
from jax import lax
from jax.experimental import pallas as pl
from jax.experimental.pallas import tpu as pltpu
from jax.sharding import PartitionSpec as P


phase_modulus = 1048576
epsilon = 1e-06
grid_half = 32
lefts = grid_half // 4
lane = 128
vmem_limit = 32 * 1024 * 1024


def cos_sin(index):
    shift = 33 - (2 * phase_modulus).bit_length()
    rest = (index << shift) >> shift
    x = rest.astype(jnp.float32) * (math.pi / (4 * phase_modulus))
    y = x * x
    sin = x + x * y * (-1.6666654611e-1 + y * (8.3321608736e-3 + y * -1.9515295891e-4))
    cos = 1 - 0.5 * y + y * y * (4.166664568298827e-2 + y * (-1.388731625493765e-3 + y * 2.443315711809948e-5))
    for _ in range(2):
        twice = sin + sin
        cos, sin = 1 - twice * sin, twice * cos
    return cos, sin


def rotate(one, two):
    return one[0] * two[0] - one[1] * two[1], one[1] * two[0] + one[0] * two[1]


def sums_kernel(
    spectra_hbm, coords_hbm, slow_hbm, sums_ref, spectra_ref, coords_ref, turn_ref, pick_ref, wanted_ref, slow_ref, arrived, small
):
    _, bins, _, width = spectra_ref.shape
    slow_copy = pltpu.make_async_copy(slow_hbm, slow_ref, small.at[0])
    coords_copy = pltpu.make_async_copy(coords_hbm, coords_ref, small.at[1])
    slow_copy.start()
    coords_copy.start()
    piece = math.gcd(bins, 8)
    copies = []
    for i in range(0, bins, piece):
        at = (slice(None), pl.ds(i, piece))
        copies.append(pltpu.make_async_copy(spectra_hbm.at[at], spectra_ref.at[at], arrived.at[i // piece]))
        copies[-1].start()

    slow_copy.wait()
    beams = slow_ref.shape[1]
    columns = 4 * grid_half
    block = math.gcd(beams, 2 * lane)
    for i in range(0, beams, block):
        at = pl.ds(i, block)
        east = 2 * slow_ref[0:1, at] + 1
        north = slow_ref[1:2, at]
        size = jnp.abs(east)
        place = (size & 7) >> 1
        positive = east > 0
        same = positive == (place >= 2)
        column = jnp.where(same, north + grid_half, grid_half - 1 - north)
        column += jnp.where((place == 1) | (place == 2), 0, 2 * grid_half)
        sign = jnp.where(place >= 2, jnp.where(positive, 0, 1), jnp.where(positive, 2, 3))
        wanted_ref[0:1, at] = sign * lefts + (size >> 3)
        pick = lax.broadcasted_iota(jnp.int32, (columns, block), 0) == column
        pick_ref[:, at] = jnp.where(pick, 1.0, 0.0).astype(jnp.bfloat16)

    coords_copy.wait()
    mine = pl.ds(pl.multiple_of(lax.axis_index("sta") * width, lane), width)
    both = coords_ref[0:1, mine] + coords_ref[1:2, mine]
    for i in range(0, bins, piece):
        number = lax.axis_index("bins") * bins + (i + 1) + lax.broadcasted_iota(jnp.int32, (piece, width), 0)
        for part, values in enumerate(cos_sin(number * both)):
            turn_ref[part, pl.ds(i, piece), :] = values

    total = 0.0
    for i in range(0, bins, piece):
        copies[i // piece].wait()
        for f in range(i, i + piece):
            for c in range(2):
                values = spectra_ref[c, f].astype(jnp.float32)
                total += values * values
    sums_ref[...] = total


def sums(spectra, coords, slowness):
    _, bins, segs, width = spectra.shape
    beams = slowness.shape[1]
    hbm = pl.BlockSpec(memory_space=pltpu.HBM)
    vmem = pl.BlockSpec(memory_space=pltpu.VMEM)
    return pl.pallas_call(
        sums_kernel,
        out_shape=(
            jax.ShapeDtypeStruct((segs, width), jnp.float32),
            jax.ShapeDtypeStruct(spectra.shape, spectra.dtype),
            jax.ShapeDtypeStruct(coords.shape, coords.dtype),
            jax.ShapeDtypeStruct((2, bins, width), jnp.float32),
            jax.ShapeDtypeStruct((4 * grid_half, beams), jnp.bfloat16),
            jax.ShapeDtypeStruct((1, beams), jnp.int32),
        ),
        in_specs=[hbm] * 3,
        out_specs=(vmem,) * 6,
        scratch_shapes=[
            pltpu.VMEM(slowness.shape, slowness.dtype),
            pltpu.SemaphoreType.DMA((bins // math.gcd(bins, 8),)),
            pltpu.SemaphoreType.DMA((2,)),
        ],
        compiler_params=pltpu.CompilerParams(vmem_limit_bytes=vmem_limit),
        cost_estimate=pl.CostEstimate(flops=2 * spectra.size, bytes_accessed=2 * spectra.size, transcendentals=0),
        name="sums",
    )(*(pltpu.with_memory_space_constraint(a, pltpu.HBM) for a in (spectra, coords, slowness)))


def tables_kernel(groups, bins_dev, coords_ref, right_ref, factor_ref, rows_ref):
    bins, _, stations = right_ref.shape
    first = lax.axis_index("bins") * bins_dev + 1
    first += lax.axis_index("sta") // (lax.axis_size("sta") // groups) * bins
    step = math.gcd(stations, 2 * lane)
    sub = lax.broadcasted_iota(jnp.int32, (8, step), 0)
    odd = (sub & 1) == 1

    @pl.loop(0, stations // step)
    def _(block):
        at = pl.ds(pl.multiple_of(block * step, step), step)
        east = jnp.broadcast_to(coords_ref[0:1, at], (8, step))
        north = jnp.broadcast_to(coords_ref[1:2, at], (8, step))
        for i in range(0, 2 * bins, 8):
            index = jnp.where(odd, 2 * east, 16 * north) * (first + i // 2 + (sub >> 1))
            for part, values in enumerate(cos_sin(index)):
                rows_ref[part, pl.ds(i, 8), :] = values
        start_unit = east + north * (2 * sub + (1 - 2 * grid_half))
        factor_unit = east * (8 * sub + 4)
        start, factor = cos_sin(start_unit * first), cos_sin(factor_unit * first)
        if bins > 1:
            start_unit, factor_unit = cos_sin(start_unit), cos_sin(factor_unit)
        for f in range(bins):
            if f > 0:
                start, factor = rotate(start, start_unit), rotate(factor, factor_unit)
            sixteen, two_east = (
                tuple(jnp.broadcast_to(rows_ref[part, r:r + 1, :], (8, step)) for part in range(2))
                for r in (2 * f, 2 * f + 1)
            )
            factor_ref[f, :, at] = jnp.concatenate(factor, 0)
            twice = 2 * sixteen[0]
            second = rotate(start, sixteen)
            for d, (one, two) in enumerate(((start, second), (rotate(start, two_east), rotate(second, two_east)))):
                for i in range(0, 2 * grid_half, 16):
                    for part in range(2):
                        rows = pl.ds((2 * part + d) * 2 * grid_half + i, 16)
                        right_ref[f, rows, at] = jnp.concatenate([one[part], two[part]], 0).astype(jnp.bfloat16)
                    one = tuple(twice * b - a for a, b in zip(one, two))
                    two = tuple(twice * b - a for a, b in zip(two, one))


def tables(coords, bins, groups, bins_dev):
    stations = coords.shape[1]
    vmem = pl.BlockSpec(memory_space=pltpu.VMEM)
    return pl.pallas_call(
        lambda *refs: tables_kernel(groups, bins_dev, *refs),
        out_shape=(
            jax.ShapeDtypeStruct((bins, 8 * grid_half, stations), jnp.bfloat16),
            jax.ShapeDtypeStruct((bins, 2 * lefts, stations), jnp.float32),
        ),
        in_specs=[vmem],
        out_specs=(vmem,) * 2,
        scratch_shapes=[pltpu.VMEM((2, 8 * pl.cdiv(bins, 4), math.gcd(stations, 2 * lane)), jnp.float32)],
        compiler_params=pltpu.CompilerParams(vmem_limit_bytes=vmem_limit),
        cost_estimate=pl.CostEstimate(flops=bins * stations * 4096, bytes_accessed=bins * stations * 576, transcendentals=0),
        name="tables",
    )(coords)


def whiten_kernel(total_bins, spectra_ref, turn_ref, *refs):
    *sums_refs, out_ref = refs
    groups, bins, rows, width = out_ref.shape
    total = sum(ref[...] for ref in sums_refs)
    inverse = 1.0 / jnp.sqrt(total / (2 * total_bins) + epsilon)
    for i in range(groups * bins):
        wr = spectra_ref[0, i].astype(jnp.float32) * inverse
        wi = spectra_ref[1, i].astype(jnp.float32) * inverse
        cos, sin = turn_ref[0, i:i + 1, :], turn_ref[1, i:i + 1, :]
        both = jnp.concatenate([wr * cos - wi * sin, wi * cos + wr * sin], 0)
        out_ref[i // bins, i % bins] = both.astype(jnp.bfloat16)


def whiten(spectra, turn, partial, total_bins, groups):
    _, bins_dev, segs, width = spectra.shape
    vmem = pl.BlockSpec(memory_space=pltpu.VMEM)
    return pl.pallas_call(
        lambda *refs: whiten_kernel(total_bins, *refs),
        out_shape=jax.ShapeDtypeStruct((groups, bins_dev // groups, 2 * segs, width), jnp.bfloat16),
        in_specs=[vmem] * (2 + len(partial)),
        out_specs=vmem,
        compiler_params=pltpu.CompilerParams(vmem_limit_bytes=vmem_limit),
        cost_estimate=pl.CostEstimate(flops=8 * spectra.size, bytes_accessed=4 * spectra.size, transcendentals=0),
        name="whiten",
    )(spectra, turn, *partial)


def grid_kernel(white_ref, right_ref, factor_ref, pick_ref, wanted_ref, out_ref, left, power):
    sources, bins, rows, width = white_ref.shape
    segs = rows // 2
    basis = 2 * lefts
    step = math.gcd(width, 2 * lane)
    norm = 1.0 / (sources * width * segs)
    columns = 4 * grid_half

    def build(f, src):
        for t in range(width // step):
            at = pl.ds(src * width + t * step, step)
            white = white_ref[src, f, :, pl.ds(t * step, step)].astype(jnp.float32)
            factor = factor_ref[f, :, at].astype(jnp.float32)
            for r in range(rows):
                value = jnp.broadcast_to(white[r:r + 1], (basis, step))
                left[f, pl.ds(basis * r, basis), at] = (factor * value).astype(jnp.bfloat16)

    def finish(f, total):
        found = [0.0] * 4
        for g in range(segs):
            real = total[basis * g:basis * (g + 1)]
            imag = total[basis * (segs + g):basis * (segs + g + 1)]
            rcc, rcs = real[:lefts, :columns], real[:lefts, columns:]
            rsc, rss = real[lefts:, :columns], real[lefts:, columns:]
            icc, ics = imag[:lefts, :columns], imag[:lefts, columns:]
            isc, iss = imag[lefts:, :columns], imag[lefts:, columns:]
            same = (rcc - rss, isc + ics, icc - iss, rsc + rcs)
            mixed = (rcc + rss, isc - ics, icc + iss, rsc - rcs)
            for q, (a, b, c, d) in ((0, same), (2, mixed)):
                found[q] += (a + b) * (a + b) + (c - d) * (c - d)
                found[q + 1] += (a - b) * (a - b) + (c + d) * (c + d)
        for q in range(4):
            power[pl.ds((4 * f + q) * lefts, lefts), :] = found[q] * norm

    dests, _, beams = out_ref.shape

    for f in range(0, bins, 2):
        both = range(f, min(f + 2, bins))
        totals = [0.0] * len(both)
        for src in range(sources):
            for i in both:
                build(i, src)
            at = pl.ds(src * width, width)
            for i in both:
                totals[i - f] += lax.dot_general(
                    left[i, :, at], right_ref[i, :, at], (((1,), (1,)), ((), ())), preferred_element_type=jnp.float32
                )
        for i in both:
            finish(i, totals[i - f])

    values = power[...]
    high = values.astype(jnp.bfloat16)
    low = (values - high.astype(jnp.float32)).astype(jnp.bfloat16)
    pair = jnp.concatenate([high, low], 1)
    for d in range(dests):
        at = pl.ds(d * beams, beams)
        pick = pick_ref[:, at]
        found = jnp.dot(pair, jnp.concatenate([pick, pick], 0), preferred_element_type=jnp.float32)
        row = lax.broadcasted_iota(jnp.int32, (4 * lefts, beams), 0) == wanted_ref[0:1, at]
        for f in range(bins):
            part = jnp.where(row, found[f * 4 * lefts:(f + 1) * 4 * lefts], 0.0)
            out_ref[d, pl.ds(f, 1), :] = jnp.sum(part, axis=0, keepdims=True)


def beam_grid(white, right, factor, pick, wanted, dests):
    sources, bins, rows, width = white.shape
    stations = sources * width
    beams = pick.shape[1] // dests
    vmem = pl.BlockSpec(memory_space=pltpu.VMEM)
    return pl.pallas_call(
        grid_kernel,
        out_shape=jax.ShapeDtypeStruct((dests, bins, beams), jnp.float32),
        in_specs=[vmem] * 5,
        out_specs=vmem,
        scratch_shapes=[
            pltpu.VMEM((bins, 2 * lefts * rows, stations), jnp.bfloat16),
            pltpu.VMEM((bins * 4 * lefts, 4 * grid_half), jnp.float32),
        ],
        compiler_params=pltpu.CompilerParams(vmem_limit_bytes=vmem_limit),
        cost_estimate=pl.CostEstimate(flops=bins * stations * 4096, bytes_accessed=bins * stations * 576, transcendentals=0),
        name="beam_grid",
    )(white, right, factor, pick, wanted)


def local(spectra, coords, slowness):
    _, bins_dev, _, width = spectra.shape
    peers = lax.axis_size("sta")
    rows = lax.axis_size("bins")
    groups = math.gcd(bins_dev, peers)
    copies = peers // groups
    bins_own = bins_dev // groups
    local_sq, spectra, coords, turn, pick, wanted = sums(spectra, coords, slowness)
    partial = [local_sq]
    if rows & (rows - 1) == 0:
        for k in (1 << i for i in range(rows.bit_length() - 1)):
            total = sum(partial)
            partial = [total, lax.ppermute(total, "bins", [(i, i ^ k) for i in range(rows)])]
    else:
        for shift in range(1, rows):
            partial.append(lax.ppermute(local_sq, "bins", [(i, (i + shift) % rows) for i in range(rows)]))
    right, factor = tables(coords, bins_own, groups, bins_dev)
    parts = whiten(spectra, turn, partial, bins_dev * rows, groups)
    if copies > 1:
        parts = jnp.repeat(parts, copies, axis=0)
    parts, right, factor = lax.optimization_barrier((parts, right, factor))
    white = lax.all_to_all(parts, "sta", 0, 0, tiled=True)
    powers = beam_grid(white, right, factor, pick, wanted, peers)
    powers = lax.all_to_all(powers, "sta", 0, 0, tiled=True)
    return powers[::copies].reshape(bins_dev, -1)


def solution(mesh):
    in_specs = (P(None, "bins", None, "sta"), P(), P())
    out_specs = P("bins", "sta")
    return jax.shard_map(local, mesh=mesh, in_specs=in_specs, out_specs=out_specs, check_vma=False)
```

```python
import math

import jax
import jax.numpy as jnp
from jax import lax
from jax.experimental import pallas as pl
from jax.experimental.pallas import tpu as pltpu
from jax.sharding import PartitionSpec as P


phase_modulus = 1048576
epsilon = 1e-06
grid_half = 32
lefts = grid_half // 4
lane = 128
vmem_limit = 32 * 1024 * 1024


def cos_sin(index):
    shift = 33 - (2 * phase_modulus).bit_length()
    rest = (index << shift) >> shift
    x = rest.astype(jnp.float32) * (math.pi / (4 * phase_modulus))
    y = x * x
    sin = x + x * y * (-1.6666654611e-1 + y * (8.3321608736e-3 + y * -1.9515295891e-4))
    cos = 1 - 0.5 * y + y * y * (4.166664568298827e-2 + y * (-1.388731625493765e-3 + y * 2.443315711809948e-5))
    for _ in range(2):
        twice = sin + sin
        cos, sin = 1 - twice * sin, twice * cos
    return cos, sin


def rotate(one, two):
    return one[0] * two[0] - one[1] * two[1], one[1] * two[0] + one[0] * two[1]


def sums_kernel(
    spectra_hbm, coords_hbm, slow_hbm, sums_ref, spectra_ref, coords_ref, turn_ref, pick_ref, wanted_ref, slow_ref, arrived, small
):
    _, bins, _, width = spectra_ref.shape
    slow_copy = pltpu.make_async_copy(slow_hbm, slow_ref, small.at[0])
    coords_copy = pltpu.make_async_copy(coords_hbm, coords_ref, small.at[1])
    slow_copy.start()
    coords_copy.start()
    piece = math.gcd(bins, 8)
    copies = []
    for i in range(0, bins, piece):
        at = (slice(None), pl.ds(i, piece))
        copies.append(pltpu.make_async_copy(spectra_hbm.at[at], spectra_ref.at[at], arrived.at[i // piece]))
        copies[-1].start()

    slow_copy.wait()
    beams = slow_ref.shape[1]
    columns = 4 * grid_half
    block = math.gcd(beams, 2 * lane)
    for i in range(0, beams, block):
        at = pl.ds(i, block)
        east = 2 * slow_ref[0:1, at] + 1
        north = slow_ref[1:2, at]
        size = jnp.abs(east)
        place = (size & 7) >> 1
        positive = east > 0
        same = positive == (place >= 2)
        column = jnp.where(same, north + grid_half, grid_half - 1 - north)
        column += jnp.where((place == 1) | (place == 2), 0, 2 * grid_half)
        sign = jnp.where(place >= 2, jnp.where(positive, 0, 1), jnp.where(positive, 2, 3))
        wanted_ref[0:1, at] = sign * lefts + (size >> 3)
        pick = lax.broadcasted_iota(jnp.int32, (columns, block), 0) == column
        pick_ref[:, at] = jnp.where(pick, 1.0, 0.0).astype(jnp.bfloat16)

    coords_copy.wait()
    mine = pl.ds(pl.multiple_of(lax.axis_index("sta") * width, lane), width)
    both = coords_ref[0:1, mine] + coords_ref[1:2, mine]
    for i in range(0, bins, piece):
        number = lax.axis_index("bins") * bins + (i + 1) + lax.broadcasted_iota(jnp.int32, (piece, width), 0)
        for part, values in enumerate(cos_sin(number * both)):
            turn_ref[part, pl.ds(i, piece), :] = values

    total = 0.0
    for i in range(0, bins, piece):
        copies[i // piece].wait()
        for f in range(i, i + piece):
            for c in range(2):
                values = spectra_ref[c, f].astype(jnp.float32)
                total += values * values
    sums_ref[...] = total


def sums(spectra, coords, slowness):
    _, bins, segs, width = spectra.shape
    beams = slowness.shape[1]
    hbm = pl.BlockSpec(memory_space=pltpu.HBM)
    vmem = pl.BlockSpec(memory_space=pltpu.VMEM)
    return pl.pallas_call(
        sums_kernel,
        out_shape=(
            jax.ShapeDtypeStruct((segs, width), jnp.float32),
            jax.ShapeDtypeStruct(spectra.shape, spectra.dtype),
            jax.ShapeDtypeStruct(coords.shape, coords.dtype),
            jax.ShapeDtypeStruct((2, bins, width), jnp.float32),
            jax.ShapeDtypeStruct((4 * grid_half, beams), jnp.bfloat16),
            jax.ShapeDtypeStruct((1, beams), jnp.int32),
        ),
        in_specs=[hbm] * 3,
        out_specs=(vmem,) * 6,
        scratch_shapes=[
            pltpu.VMEM(slowness.shape, slowness.dtype),
            pltpu.SemaphoreType.DMA((bins // math.gcd(bins, 8),)),
            pltpu.SemaphoreType.DMA((2,)),
        ],
        compiler_params=pltpu.CompilerParams(vmem_limit_bytes=vmem_limit),
        cost_estimate=pl.CostEstimate(flops=2 * spectra.size, bytes_accessed=2 * spectra.size, transcendentals=0),
        name="sums",
    )(*(pltpu.with_memory_space_constraint(a, pltpu.HBM) for a in (spectra, coords, slowness)))


def tables_kernel(groups, bins_dev, coords_ref, right_ref, factor_ref, rows_ref):
    bins, _, stations = right_ref.shape
    first = lax.axis_index("bins") * bins_dev + 1
    first += lax.axis_index("sta") // (lax.axis_size("sta") // groups) * bins
    step = math.gcd(stations, 2 * lane)
    sub = lax.broadcasted_iota(jnp.int32, (8, step), 0)
    odd = (sub & 1) == 1

    @pl.loop(0, stations // step)
    def _(block):
        at = pl.ds(pl.multiple_of(block * step, step), step)
        east = jnp.broadcast_to(coords_ref[0:1, at], (8, step))
        north = jnp.broadcast_to(coords_ref[1:2, at], (8, step))
        for i in range(0, 2 * bins, 8):
            index = jnp.where(odd, 2 * east, 16 * north) * (first + i // 2 + (sub >> 1))
            for part, values in enumerate(cos_sin(index)):
                rows_ref[part, pl.ds(i, 8), :] = values
        start_unit = east + north * (2 * sub + (1 - 2 * grid_half))
        factor_unit = east * (8 * sub + 4)
        start, factor = cos_sin(start_unit * first), cos_sin(factor_unit * first)
        if bins > 1:
            start_unit, factor_unit = cos_sin(start_unit), cos_sin(factor_unit)
        for f in range(bins):
            if f > 0:
                start, factor = rotate(start, start_unit), rotate(factor, factor_unit)
            sixteen, two_east = (
                tuple(jnp.broadcast_to(rows_ref[part, r:r + 1, :], (8, step)) for part in range(2))
                for r in (2 * f, 2 * f + 1)
            )
            factor_ref[f, :, at] = jnp.concatenate(factor, 0)
            twice = 2 * sixteen[0]
            second = rotate(start, sixteen)
            for d, (one, two) in enumerate(((start, second), (rotate(start, two_east), rotate(second, two_east)))):
                for i in range(0, 2 * grid_half, 16):
                    for part in range(2):
                        rows = pl.ds((2 * part + d) * 2 * grid_half + i, 16)
                        right_ref[f, rows, at] = jnp.concatenate([one[part], two[part]], 0).astype(jnp.bfloat16)
                    one = tuple(twice * b - a for a, b in zip(one, two))
                    two = tuple(twice * b - a for a, b in zip(two, one))


def tables(coords, bins, groups, bins_dev):
    stations = coords.shape[1]
    vmem = pl.BlockSpec(memory_space=pltpu.VMEM)
    return pl.pallas_call(
        lambda *refs: tables_kernel(groups, bins_dev, *refs),
        out_shape=(
            jax.ShapeDtypeStruct((bins, 8 * grid_half, stations), jnp.bfloat16),
            jax.ShapeDtypeStruct((bins, 2 * lefts, stations), jnp.float32),
        ),
        in_specs=[vmem],
        out_specs=(vmem,) * 2,
        scratch_shapes=[pltpu.VMEM((2, 8 * pl.cdiv(bins, 4), math.gcd(stations, 2 * lane)), jnp.float32)],
        compiler_params=pltpu.CompilerParams(vmem_limit_bytes=vmem_limit),
        cost_estimate=pl.CostEstimate(flops=bins * stations * 4096, bytes_accessed=bins * stations * 576, transcendentals=0),
        name="tables",
    )(coords)


def whiten_kernel(total_bins, spectra_ref, turn_ref, *refs):
    *sums_refs, out_ref = refs
    groups, bins, rows, width = out_ref.shape
    total = sum(ref[...] for ref in sums_refs)
    inverse = 1.0 / jnp.sqrt(total / (2 * total_bins) + epsilon)
    for i in range(groups * bins):
        wr = spectra_ref[0, i].astype(jnp.float32) * inverse
        wi = spectra_ref[1, i].astype(jnp.float32) * inverse
        cos, sin = turn_ref[0, i:i + 1, :], turn_ref[1, i:i + 1, :]
        both = jnp.concatenate([wr * cos - wi * sin, wi * cos + wr * sin], 0)
        out_ref[i // bins, i % bins] = both.astype(jnp.bfloat16)


def whiten(spectra, turn, partial, total_bins, groups):
    _, bins_dev, segs, width = spectra.shape
    vmem = pl.BlockSpec(memory_space=pltpu.VMEM)
    return pl.pallas_call(
        lambda *refs: whiten_kernel(total_bins, *refs),
        out_shape=jax.ShapeDtypeStruct((groups, bins_dev // groups, 2 * segs, width), jnp.bfloat16),
        in_specs=[vmem] * (2 + len(partial)),
        out_specs=vmem,
        compiler_params=pltpu.CompilerParams(vmem_limit_bytes=vmem_limit),
        cost_estimate=pl.CostEstimate(flops=8 * spectra.size, bytes_accessed=4 * spectra.size, transcendentals=0),
        name="whiten",
    )(spectra, turn, *partial)


def grid_kernel(white_ref, right_ref, factor_ref, pick_ref, wanted_ref, out_ref, left, power):
    sources, bins, rows, width = white_ref.shape
    segs = rows // 2
    basis = 2 * lefts
    step = math.gcd(width, 2 * lane)
    norm = 1.0 / (sources * width * segs)
    columns = 4 * grid_half

    def build(f, src):
        for t in range(width // step):
            at = pl.ds(src * width + t * step, step)
            white = white_ref[src, f, :, pl.ds(t * step, step)].astype(jnp.float32)
            factor = factor_ref[f, :, at].astype(jnp.float32)
            for r in range(rows):
                value = jnp.broadcast_to(white[r:r + 1], (basis, step))
                left[f, pl.ds(basis * r, basis), at] = (factor * value).astype(jnp.bfloat16)

    def finish(f, total):
        found = [0.0] * 4
        for g in range(segs):
            real = total[basis * g:basis * (g + 1)]
            imag = total[basis * (segs + g):basis * (segs + g + 1)]
            rcc, rcs = real[:lefts, :columns], real[:lefts, columns:]
            rsc, rss = real[lefts:, :columns], real[lefts:, columns:]
            icc, ics = imag[:lefts, :columns], imag[:lefts, columns:]
            isc, iss = imag[lefts:, :columns], imag[lefts:, columns:]
            same = (rcc - rss, isc + ics, icc - iss, rsc + rcs)
            mixed = (rcc + rss, isc - ics, icc + iss, rsc - rcs)
            for q, (a, b, c, d) in ((0, same), (2, mixed)):
                found[q] += (a + b) * (a + b) + (c - d) * (c - d)
                found[q + 1] += (a - b) * (a - b) + (c + d) * (c + d)
        for q in range(4):
            power[pl.ds((4 * f + q) * lefts, lefts), :] = found[q] * norm

    dests, _, beams = out_ref.shape

    for f in range(0, bins, 2):
        both = range(f, min(f + 2, bins))
        totals = [0.0] * len(both)
        for src in range(sources):
            for i in both:
                build(i, src)
            at = pl.ds(src * width, width)
            for i in both:
                totals[i - f] += lax.dot_general(
                    left[i, :, at], right_ref[i, :, at], (((1,), (1,)), ((), ())), preferred_element_type=jnp.float32
                )
        for i in both:
            finish(i, totals[i - f])

    values = power[...]
    high = values.astype(jnp.bfloat16)
    low = (values - high.astype(jnp.float32)).astype(jnp.bfloat16)
    pair = jnp.concatenate([high, low], 1)
    for d in range(dests):
        at = pl.ds(d * beams, beams)
        pick = pick_ref[:, at]
        found = jnp.dot(pair, jnp.concatenate([pick, pick], 0), preferred_element_type=jnp.float32)
        row = lax.broadcasted_iota(jnp.int32, (4 * lefts, beams), 0) == wanted_ref[0:1, at]
        part = jnp.where(row[None], found.reshape(bins, 4 * lefts, beams), 0.0)
        out_ref[d] = jnp.sum(part, axis=1)


def beam_grid(white, right, factor, pick, wanted, dests):
    sources, bins, rows, width = white.shape
    stations = sources * width
    beams = pick.shape[1] // dests
    vmem = pl.BlockSpec(memory_space=pltpu.VMEM)
    return pl.pallas_call(
        grid_kernel,
        out_shape=jax.ShapeDtypeStruct((dests, bins, beams), jnp.float32),
        in_specs=[vmem] * 5,
        out_specs=vmem,
        scratch_shapes=[
            pltpu.VMEM((bins, 2 * lefts * rows, stations), jnp.bfloat16),
            pltpu.VMEM((bins * 4 * lefts, 4 * grid_half), jnp.float32),
        ],
        compiler_params=pltpu.CompilerParams(vmem_limit_bytes=vmem_limit),
        cost_estimate=pl.CostEstimate(flops=bins * stations * 4096, bytes_accessed=bins * stations * 576, transcendentals=0),
        name="beam_grid",
    )(white, right, factor, pick, wanted)


def local(spectra, coords, slowness):
    _, bins_dev, _, width = spectra.shape
    peers = lax.axis_size("sta")
    rows = lax.axis_size("bins")
    groups = math.gcd(bins_dev, peers)
    copies = peers // groups
    bins_own = bins_dev // groups
    local_sq, spectra, coords, turn, pick, wanted = sums(spectra, coords, slowness)
    partial = [local_sq]
    if rows & (rows - 1) == 0:
        for k in (1 << i for i in range(rows.bit_length() - 1)):
            total = sum(partial)
            partial = [total, lax.ppermute(total, "bins", [(i, i ^ k) for i in range(rows)])]
    else:
        for shift in range(1, rows):
            partial.append(lax.ppermute(local_sq, "bins", [(i, (i + shift) % rows) for i in range(rows)]))
    right, factor = tables(coords, bins_own, groups, bins_dev)
    parts = whiten(spectra, turn, partial, bins_dev * rows, groups)
    if copies > 1:
        parts = jnp.repeat(parts, copies, axis=0)
    parts, right, factor = lax.optimization_barrier((parts, right, factor))
    white = lax.all_to_all(parts, "sta", 0, 0, tiled=True)
    powers = beam_grid(white, right, factor, pick, wanted, peers)
    powers = lax.all_to_all(powers, "sta", 0, 0, tiled=True)
    return powers[::copies].reshape(bins_dev, -1)


def solution(mesh):
    in_specs = (P(None, "bins", None, "sta"), P(), P())
    out_specs = P("bins", "sta")
    return jax.shard_map(local, mesh=mesh, in_specs=in_specs, out_specs=out_specs, check_vma=False)
```
